16 devices in a mesh: dp: 2 (over y, z), tp: 8 (over x, core).
Axes of the slice: x: 4, y: 2, z: 1, core: 2. Of those that a mesh axis runs over, the one named last changes fastest.
The devices are a block of a 4x4x8 slice.
Arguments:
- x: bfloat16 [2048, 9216], P(('dp', 'tp')), parts along dimension 0
- gain: bfloat16 [9216], replicated
- wq: bfloat16 [9216, 9216], P(None, 'tp')
- wk: bfloat16 [9216, 9216], P(None, 'tp')
- wv: bfloat16 [9216, 9216], P(None, 'tp')
- wo: bfloat16 [9216, 9216], P('tp')
Outputs:
- output: bfloat16 [2048, 9216], P(('dp', 'tp')), parts along dimension 0
There are 2 independent parts. The reference program is written for one: setup_inputs(seed, part) draws one part's arguments, and reference() takes and returns one part's arrays. A program takes and returns all parts, laid end to end along the dimension named above; an argument that names none is the same for every part.
All inputs are finite; a program needn't handle non-finite values.
Results may differ from the reference program's by a relative error of at most 0.012.
Values are sent between devices in bfloat16 or wider.
A program may use at most 768 MiB of HBM per device.

```python
import jax
import jax.numpy as jnp
from jax import lax

ROWS = 1024
D = 9216
HEADS = 72
KV_HEADS = 72
HEAD = 128
THETA = 10000


def setup_inputs(seed: int = 0, part: int = 0) -> dict:
    kx, kn, kq, kk, kv, ko = jax.random.split(jax.random.key(seed), 6)

    def weights(key, rows, columns):
        return jax.random.normal(key, (rows, columns), jnp.float32) * rows**-0.5

    drawn = {
        "x": jax.random.normal(jax.random.fold_in(kx, part), (ROWS, D), jnp.float32),
        "gain": 1 + 0.1 * jax.random.normal(kn, (D,), jnp.float32),
        "wq": 2 * weights(kq, D, HEADS * HEAD),
        "wk": 2 * weights(kk, D, KV_HEADS * HEAD),
        "wv": 4 * weights(kv, D, KV_HEADS * HEAD),
        "wo": weights(ko, HEADS * HEAD, D),
    }
    return {k: v.astype(jnp.bfloat16) for k, v in drawn.items()}


def normed(x, gain):
    wide = x.astype(jnp.float32)
    scale = lax.rsqrt(jnp.mean(wide * wide, -1, keepdims=True) + 1e-6)
    return (wide * scale * gain.astype(jnp.float32)).astype(jnp.bfloat16)


def turned(t, place, theta):
    half = t.shape[-1] // 2
    angle = place.astype(jnp.float32)[:, None] * theta ** (-jnp.arange(half, dtype=jnp.float32) / half)
    cos, sin = jnp.cos(angle)[:, None], jnp.sin(angle)[:, None]
    a, b = t[..., :half].astype(jnp.float32), t[..., half:].astype(jnp.float32)
    return jnp.concatenate([a * cos - b * sin, b * cos + a * sin], -1).astype(jnp.bfloat16)


def matmul(a, w):
    return jnp.dot(a, w, preferred_element_type=jnp.float32).astype(jnp.bfloat16)


def einsum(form, a, b):
    return jnp.einsum(form, a.astype(jnp.float32), b.astype(jnp.float32))


def attention(q, k, v):
    scores = einsum("tgsd,ugd->gstu", q, k) * q.shape[-1] ** -0.5
    token = jnp.arange(q.shape[0])
    scores = jnp.where(token[:, None] >= token, scores, -jnp.inf)
    weights = jax.nn.softmax(scores, -1).astype(jnp.bfloat16)
    return einsum("gstu,ugd->tgsd", weights, v).astype(jnp.bfloat16)


def reference(x, gain, wq, wk, wv, wo):
    a, place = normed(x, gain), jnp.arange(ROWS)
    q = turned(matmul(a, wq).reshape(ROWS, HEADS, HEAD), place, THETA).reshape(ROWS, KV_HEADS, -1, HEAD)
    k = turned(matmul(a, wk).reshape(ROWS, KV_HEADS, HEAD), place, THETA)
    v = matmul(a, wv).reshape(ROWS, KV_HEADS, HEAD)
    seen = attention(q, k, v).reshape(ROWS, HEADS * HEAD)
    return (x.astype(jnp.float32) + jnp.dot(seen, wo, preferred_element_type=jnp.float32)).astype(jnp.bfloat16)
```

```python
import functools

import jax
import jax.numpy as jnp
import numpy as np
from jax import lax
from jax.experimental import pallas as pl
from jax.experimental.pallas import tpu as pltpu
from jax.sharding import PartitionSpec as P

HEAD = 128
THETA = 10000
LOG2E = 1.4426950408889634
HIDDEN = -2e30
VMEM = 63 * 2**20
CORES = 2
TILE = 1024
SLOTS = 3
LAG = 2
MESH = pl.DeviceIdType.MESH
f32, bf16 = jnp.float32, jnp.bfloat16

PASS, IN1, IN2 = 512, 640, 768


def rotation(rows):
    half = HEAD // 2
    angle = np.arange(rows, dtype=np.float64)[:, None] * float(THETA) ** (-np.arange(half, dtype=np.float64) / half)
    cos, sin = np.cos(angle), np.sin(angle)
    return np.concatenate([cos, cos, -sin, sin], 1).astype(np.float32)


def kernel(n, x_ref, gain_ref, turn_ref, wq_ref, wk_ref, wv_ref, wo_ref, y_ref,
           x_s, turn_s, held, ring, acc, qkv, seen, top_s, mix_s,
           in_sem, w_sem, wo_sem, y_sem, ag_send, ag_recv, ex_send, ex_recv, rs_send, rs_recv, free):
    me = lax.axis_index("tp")
    chips = n // CORES
    chip, core = me // CORES, me % CORES
    chip_at = lambda ahead: lax.rem(chip + ahead, chips)
    partner = chip * CORES + 1 - core
    right, left = chip_at(1) * CORES + core, chip_at(chips - 1) * CORES + core
    own = pl.multiple_of(core * 128, 128)
    tiles = x_ref.shape[1] // TILE
    width = wq_ref.shape[1]
    heads = width // HEAD

    def cols(j, size=TILE):
        return pl.ds(pl.multiple_of(j * size, 128), size)

    def weights(j):
        slot = lax.rem(j, SLOTS)
        rows = pl.ds(pl.multiple_of(slot * TILE, TILE), TILE)
        return [pltpu.make_async_copy(w.at[cols(j), :], ring.at[rows, pl.ds(m * width, width)], w_sem.at[slot, m])
                for m, w in enumerate((wq_ref, wk_ref, wv_ref))]

    def wo_slot(i):
        slot = lax.rem(i, 6)
        return pl.ds(pl.multiple_of(lax.rem(slot, 2) * width, 128), width), cols(slot // 2)

    def wo_tile(i):
        rows, columns = wo_slot(i)
        return pltpu.make_async_copy(wo_ref.at[:, cols(lax.rem(i, tiles))], ring.at[rows, columns], wo_sem.at[lax.rem(i, 6)])

    def gather(kind, j):
        at, to, size, device = [
            (own, own, 128, partner),
            (own, 256 + own, 128, right),
            (own, 512 + own, 128, left),
            (256 + own, 256 + own, 128, partner),
            (512 + own, 512 + own, 128, partner),
            (256 + own, 768 + own, 64, right),
            (512 + own + 64, 768 + own + 64, 64, left),
            (768 + own, 768 + own, 64, partner),
            (768 + own + 64, 768 + own + 64, 64, partner),
        ][kind]
        rows = lambda r: pl.ds(pl.multiple_of(r, 64), size)
        return pltpu.make_async_remote_copy(
            src_ref=held.at[j, rows(at), :], dst_ref=held.at[j, rows(to), :], send_sem=ag_send.at[kind, j], recv_sem=ag_recv.at[kind, j],
            device_id={"tp": device}, device_id_type=MESH)

    def exchange(b, j):
        return pltpu.make_async_remote_copy(
            src_ref=held.at[j, pl.ds(PASS, 128), :], dst_ref=held.at[j, pl.ds(pl.multiple_of(b * 128, 128), 128), :],
            send_sem=ex_send.at[b, j], recv_sem=ex_recv.at[b, j], device_id={"tp": partner}, device_id_type=MESH)

    def onwards(kind, j):
        at, to, device = [
            (0, IN1, right),
            (64, IN1 + 64, left),
            (128 + 64, IN2 + 64, right),
            (256, IN2 + 128, left),
            (128, IN2, right),
            (256 + 64, IN2 + 128 + 64, left),
        ][kind]
        return pltpu.make_async_remote_copy(
            src_ref=held.at[j, pl.ds(at, 64), :], dst_ref=held.at[j, pl.ds(to, 64), :], send_sem=rs_send.at[kind, j],
            recv_sem=rs_recv.at[kind, j], device_id={"tp": device}, device_id_type=MESH)

    def out(j):
        return pltpu.make_async_copy(held.at[j, pl.ds(PASS, 128), :], y_ref.at[:, cols(j)], y_sem.at[j])

    fetch = pltpu.make_async_copy(x_ref, x_s, in_sem.at[0])
    fetch.start()
    for j in range(SLOTS):
        for copy in weights(j):
            copy.start()
    fetch_turn = pltpu.make_async_copy(turn_ref, turn_s, in_sem.at[1])
    fetch_turn.start()
    barrier = pltpu.get_barrier_semaphore()
    for device in (partner, right, left):
        pl.semaphore_signal(barrier, inc=1, device_id={"tp": device}, device_id_type=MESH)
    fetch.wait()
    total = jnp.zeros((128, 128), f32)
    for j in range(tiles):
        wide = x_s[:, j * TILE : (j + 1) * TILE].astype(f32)
        square = wide * wide
        for m in range(0, TILE, 128):
            total = total + square[:, m : m + 128]
    scale = lax.rsqrt(jnp.sum(total, -1, keepdims=True) / x_ref.shape[1] + 1e-6)
    pl.semaphore_wait(barrier, 3)

    def norm(j, _):
        wide = x_s[:, cols(j)].astype(f32)
        held[j, pl.ds(own, 128), :] = (wide * scale * gain_ref[:, cols(j)].astype(f32)).astype(bf16)
        for kind in range(3):
            gather(kind, j).start()
        return 0

    lax.fori_loop(0, tiles, norm, 0)

    def unit(j, first, size):
        slot = lax.rem(j, SLOTS)
        w = ring[pl.ds(pl.multiple_of(slot * TILE, TILE), TILE), :]
        term = jnp.dot(held[j, first : first + size, :], w, preferred_element_type=f32)
        acc[:size, :] = jnp.where(j == 0, 0.0, acc[:size, :]) + term

    def turned_heads(first, of_chip):
        rows = pl.ds(pl.multiple_of(of_chip * 256, 256), 256)

        def head(h, _):
            cos, sin = turn_s[rows, :HEAD], turn_s[rows, HEAD:]
            for m in range(3):
                t = acc[first : first + 256, cols(m * heads + h, HEAD)].astype(bf16)
                if m < 2:
                    t = t.astype(f32)
                    t = (t * cos + pltpu.roll(t, HEAD // 2, 1) * sin).astype(bf16)
                qkv[m * heads + h, rows, :] = t
            return 0

        lax.fori_loop(0, heads, head, 0)

    def neighbours(j):
        for kind in (1, 2):
            gather(kind, j).wait_recv()
        for kind in (5, 6, 3, 4):
            gather(kind, j).start()

    def far(j):
        for kind in (5, 6):
            gather(kind, j).wait_recv()
        for kind in (7, 8):
            gather(kind, j).start()

    def refill(j, more):
        @pl.when(more)
        def _():
            for copy in weights(lax.rem(j + SLOTS, tiles)):
                copy.start()

    def own_chip(j, _):
        @pl.when(j == 5)
        def _():
            neighbours(0)

        @pl.when(j == 8)
        def _():
            neighbours(1)

        gather(0, j).wait_recv()
        for copy in weights(j):
            copy.wait()
        unit(j, 0, 256)
        refill(j, True)
        return 0

    lax.fori_loop(0, tiles, own_chip, 0)
    fetch_turn.wait()
    turned_heads(0, chip)

    def both_neighbours(j, _):
        @pl.when((j > 0) & (j < tiles - 1))
        def _():
            neighbours(j + 1)

        for kind in (3, 4):
            gather(kind, j).wait_recv()
        for copy in weights(j):
            copy.wait()
        unit(j, 256, 512)
        refill(j, True)
        return 0

    lax.fori_loop(0, tiles, both_neighbours, 0)
    far(0)
    turned_heads(0, chip_at(chips - 1))
    turned_heads(256, chip_at(1))

    def far_chip(j, _):
        @pl.when(j < tiles - 1)
        def _():
            far(j + 1)

        for kind in (7, 8):
            gather(kind, j).wait_recv()
        for copy in weights(j):
            copy.wait()
        unit(j, 768, 256)
        refill(j, j + SLOTS < tiles)
        return 0

    lax.fori_loop(0, tiles, far_chip, 0)
    for i in range(6):
        wo_tile(i).start()

    def sent(j, _):
        for kind in range(9):
            gather(kind, j).wait_send()
        return 0

    lax.fori_loop(0, tiles, sent, 0)
    for i, device in enumerate((partner, right, left)):
        pl.semaphore_signal(free.at[i], inc=1, device_id={"tp": device}, device_id_type=MESH)
    turned_heads(0, chip_at(2))

    e = HEAD**-0.5 * LOG2E

    def dot(a, b, ca, cb):
        return lax.dot_general(a, b, (((ca,), (cb,)), ((), ())), preferred_element_type=f32)

    def attention(d):
        queries = pl.ds(pl.multiple_of(d * 256, 256), 256)
        ones = jnp.ones((8, 256), bf16)

        def block(j, diagonal):
            keys = pl.ds(pl.multiple_of(j * 256, 256), 256)
            scores = [dot(qkv[heads + h, keys, :], qkv[h, queries, :], 1, 1) for h in range(heads)]
            weights, keeps = [], []
            for h, s in enumerate(scores):
                if diagonal:
                    s = jnp.where(lax.broadcasted_iota(jnp.int32, (256, 256), 1) >= lax.broadcasted_iota(jnp.int32, (256, 256), 0), s, HIDDEN)
                top = s.max(axis=0, keepdims=True)
                if not diagonal:
                    old = top_s[h : h + 1, :]
                    top = jnp.maximum(old, top)
                    keeps.append(jnp.exp2((old - top) * e))
                top_s[h : h + 1, :] = top
                weights.append(jnp.exp2((s - top) * e).astype(bf16))
            for h, p in enumerate(weights):
                values = jnp.concatenate([qkv[2 * heads + h, keys, :].T, ones], axis=0)
                got = dot(values, p, 1, 0)
                mix_s[h] = got if diagonal else mix_s[h] * keeps[h] + got

        block(d, True)
        lax.fori_loop(0, d, lambda j, _: block(j, False), None)
        for h in range(heads):
            got = (mix_s[h, :HEAD, :] * (1 / mix_s[h, HEAD : HEAD + 1, :])).T.astype(bf16)
            for half in range(2):
                at = pl.multiple_of(lax.rem(core + half, 2) * 128, 128)
                seen[pl.ds(at, 128), h * HEAD : (h + 1) * HEAD] = got[half * 128 : (half + 1) * 128]

    def place(i):
        return pl.ds(pl.multiple_of(i // 3 * 64, 64), 64), cols(lax.rem(i, 3))

    def tile(b, j):
        i = b * tiles + j
        wo_tile(i).wait()
        rows, columns = wo_slot(i)
        term = jnp.dot(seen[...], ring[rows, columns], preferred_element_type=f32)

        @pl.when(b > 0)
        def _():
            exchange(b - 1, j).wait_send()

        for half in range(2):
            acc[place(18 + lax.rem(j, 3) * 2 + half)] = term[half * 64 : half * 64 + 64]
        held[j, PASS : PASS + 128, :] = term[128:].astype(bf16)
        exchange(b, j).start()

        @pl.when(i + 6 < 4 * tiles)
        def _():
            wo_tile(i + 6).start()

    def finish(b, j):
        exchange(b, j).wait_recv()
        got = held[j, pl.ds(pl.multiple_of(b * 128, 128), 128), :].astype(f32)
        low = acc[place(18 + lax.rem(j, 3) * 2)] + got[:64]
        high = acc[place(18 + lax.rem(j, 3) * 2 + 1)] + got[64:]

        @pl.when(b == 0)
        def _():
            held[j, 0:64, :] = low.astype(bf16)
            held[j, 64:128, :] = high.astype(bf16)
            onwards(0, j).start()
            onwards(1, j).start()

        @pl.when(b == 1)
        def _():
            held[j, 192:256, :] = high.astype(bf16)
            onwards(2, j).start()
            acc[place(j)] = low

        @pl.when(b == 2)
        def _():
            held[j, 256:320, :] = low.astype(bf16)
            onwards(3, j).start()
            acc[place(tiles + j)] = high

        @pl.when(b == 3)
        def _():
            acc[place(2 * j)] = low
            acc[place(2 * j + 1)] = high

    def add_and_send(j, _):
        onwards(0, j).wait_recv()
        held[j, 128:192, :] = (acc[place(j)] + held[j, IN1 : IN1 + 64, :].astype(f32)).astype(bf16)
        onwards(4, j).start()
        onwards(1, j).wait_recv()
        held[j, 320:384, :] = (acc[place(tiles + j)] + held[j, IN1 + 64 : IN1 + 128, :].astype(f32)).astype(bf16)
        onwards(5, j).start()
        return 0

    def chip_block(b, _):
        @pl.when(b == 3)
        def _():
            lax.fori_loop(0, tiles, add_and_send, 0)

        ahead = jnp.where(b == 0, 2, jnp.where(b == 1, 1, jnp.where(b == 2, chips - 1, 0)))
        attention(chip_at(ahead))

        @pl.when(b == 0)
        def _():
            for i in range(3):
                pl.semaphore_wait(free.at[i], 1)

        def step(j, _):
            @pl.when(j < tiles)
            def _():
                tile(b, j)

            @pl.when(j >= LAG)
            def _():
                finish(b, j - LAG)

            return 0

        lax.fori_loop(0, tiles + LAG, step, 0)
        return 0

    lax.fori_loop(0, 4, chip_block, 0)

    def last(j, _):
        exchange(3, j).wait_send()
        for kind in range(2, 6):
            onwards(kind, j).wait_recv()
        for half in range(2):
            rows = slice(half * 64, half * 64 + 64)
            total = acc[place(2 * j + half)]
            for side in range(2):
                at = IN2 + side * 128 + half * 64
                total = total + held[j, at : at + 64, :].astype(f32)
            held[j, PASS + half * 64 : PASS + half * 64 + 64, :] = (x_s[rows, cols(j)].astype(f32) + total).astype(bf16)
        out(j).start()
        return 0

    lax.fori_loop(0, tiles, last, 0)

    def done(j, _):
        for kind in range(6):
            onwards(kind, j).wait_send()
        out(j).wait()
        return 0

    lax.fori_loop(0, tiles, done, 0)


def solution(mesh):
    n = mesh.shape["tp"]

    def step(x, gain, wq, wk, wv, wo):
        mine, depth = x.shape
        width = wq.shape[1]
        heads, tiles, rows = width // HEAD, depth // TILE, mine * n
        anywhere = pl.BlockSpec(memory_space=pl.ANY)
        dma = pltpu.SemaphoreType.DMA
        return pl.pallas_call(
            functools.partial(kernel, n),
            out_shape=jax.ShapeDtypeStruct((mine, depth), bf16),
            in_specs=[anywhere, pl.BlockSpec(memory_space=pltpu.VMEM)] + [anywhere] * 5,
            out_specs=anywhere,
            scratch_shapes=[
                pltpu.VMEM((mine, depth), bf16),
                pltpu.VMEM((rows, 2 * HEAD), f32),
                pltpu.VMEM((tiles, rows, TILE), bf16),
                pltpu.VMEM((SLOTS * TILE, 3 * width), bf16),
                pltpu.VMEM((512, 3 * width), f32),
                pltpu.VMEM((3 * heads, rows, HEAD), bf16),
                pltpu.VMEM((256, width), bf16),
                pltpu.VMEM((16, 256), f32),
                pltpu.VMEM((heads, HEAD + 8, 256), f32),
                dma((2,)), dma((SLOTS, 3)), dma((6,)), dma((tiles,)),
                dma((9, tiles)), dma((9, tiles)), dma((4, tiles)), dma((4, tiles)), dma((6, tiles)), dma((6, tiles)),
                pltpu.SemaphoreType.REGULAR((3,)),
            ],
            compiler_params=pltpu.CompilerParams(collective_id=0, has_side_effects=True, vmem_limit_bytes=VMEM),
        )(x, gain.reshape(1, -1), jnp.asarray(rotation(rows)), wq, wk, wv, wo)

    tokens, columns = P(("dp", "tp"), None), P(None, "tp")
    return jax.shard_map(
        step,
        mesh=mesh,
        in_specs=(tokens, P(None), columns, columns, columns, P("tp", None)),
        out_specs=tokens,
        check_vma=False,
    )
```

```python
import functools

import jax
import jax.numpy as jnp
import numpy as np
from jax import lax
from jax.experimental import pallas as pl
from jax.experimental.pallas import tpu as pltpu
from jax.sharding import PartitionSpec as P

HEAD = 128
THETA = 10000
LOG2E = 1.4426950408889634
HIDDEN = -2e30
VMEM = 63 * 2**20
CORES = 2
TILE = 1024
SLOTS = 3
LAG = 2
MESH = pl.DeviceIdType.MESH
f32, bf16 = jnp.float32, jnp.bfloat16

INTO = (640, 256, 384)
EXCHANGED = (512, 768, None, 896)


def rotation(rows):
    half = HEAD // 2
    angle = np.arange(rows, dtype=np.float64)[:, None] * float(THETA) ** (-np.arange(half, dtype=np.float64) / half)
    cos, sin = np.cos(angle), np.sin(angle)
    return np.concatenate([cos, cos, -sin, sin], 1).astype(np.float32)


def pick(i, values):
    got = values[-1]
    for m in range(len(values) - 2, -1, -1):
        got = jnp.where(i == m, values[m], got)
    return got


def kernel(n, x_ref, gain_ref, turn_ref, wq_ref, wk_ref, wv_ref, wo_ref, y_ref,
           x_s, turn_s, held, ring, acc, qkv, seen, top_s, mix_s,
           in_sem, w_sem, wo_sem, y_sem, own_send, own_recv, to_send, to_recv, pass_send, pass_recv, ex_send, ex_recv, rs_send, rs_recv, free):
    me = lax.axis_index("tp")
    chips = n // CORES
    chip, core = me // CORES, me % CORES
    chip_at = lambda ahead: lax.rem(chip + ahead, chips)
    partner = chip * CORES + 1 - core
    forth, back = jnp.where(core == 0, 1, chips - 1), jnp.where(core == 0, chips - 1, 1)
    after, before = chip_at(forth) * CORES + core, chip_at(back) * CORES + core
    across = chip_at(forth) * CORES + 1 - core
    own = pl.multiple_of(core * 128, 128)
    other = pl.multiple_of((1 - core) * 128, 128)
    tiles = x_ref.shape[1] // TILE
    width = wq_ref.shape[1]
    heads = width // HEAD
    early = ((core == 0) & (chip != 0)) | ((core == 1) & (chip == chips - 1))

    def cols(j, size=TILE):
        return pl.ds(pl.multiple_of(j * size, 128), size)

    def some(r, size=128):
        return pl.ds(pl.multiple_of(r, 128), size)

    def weights(j):
        slot = lax.rem(j, SLOTS)
        return [pltpu.make_async_copy(w.at[cols(j), :], ring.at[some(slot * TILE, TILE), pl.ds(m * width, width)], w_sem.at[slot, m])
                for m, w in enumerate((wq_ref, wk_ref, wv_ref))]

    def wo_slot(i):
        slot = lax.rem(i, 6)
        return some(lax.rem(slot, 2) * width, width), cols(slot // 2)

    def wo_tile(i):
        rows, columns = wo_slot(i)
        return pltpu.make_async_copy(wo_ref.at[:, cols(lax.rem(i, tiles))], ring.at[rows, columns], wo_sem.at[lax.rem(i, 6)])

    def remote(j, at, to, send, recv, device):
        return pltpu.make_async_remote_copy(src_ref=held.at[j, some(at), :], dst_ref=held.at[j, some(to), :], send_sem=send, recv_sem=recv,
                                            device_id={"tp": device}, device_id_type=MESH)

    def own_to_partner(j):
        return remote(j, own, own, own_send.at[j], own_recv.at[j], partner)

    def message(s, j):
        first = 256 + own
        at = (own, jnp.where(early, first, other), jnp.where(early, other, first))[s]
        return remote(j, at, 256 + s * 256 + own, to_send.at[s, j], to_recv.at[s, j], after)

    def passed(s, j, core_at=own):
        return remote(j, 256 + s * 256 + core_at, 256 + s * 256 + core_at, pass_send.at[s, j], pass_recv.at[s, j], partner)

    def exchange(b, j):
        return remote(j, own, pick(b, [own if r is None else r for r in EXCHANGED]), ex_send.at[b, j], ex_recv.at[b, j], partner)

    def exchanged(b):
        return some(pick(b, [other if r is None else r for r in EXCHANGED]))

    def onwards(kind, j):
        at = (EXCHANGED[0], EXCHANGED[1], EXCHANGED[3])[kind]
        return remote(j, at, INTO[kind], rs_send.at[kind, j], rs_recv.at[kind, j], after if kind < 2 else across)

    def arrival(kind, j):
        return remote(j, EXCHANGED[0], pick(kind, INTO), rs_send.at[kind, j], rs_recv.at[kind, j], after)

    def out(j):
        return pltpu.make_async_copy(held.at[j, some(own), :], y_ref.at[:, cols(j)], y_sem.at[j])

    fetch = pltpu.make_async_copy(x_ref, x_s, in_sem.at[0])
    fetch.start()
    for j in range(SLOTS):
        for copy in weights(j):
            copy.start(priority=1)
    fetch_turn = pltpu.make_async_copy(turn_ref, turn_s, in_sem.at[1])
    fetch_turn.start()
    barrier = pltpu.get_barrier_semaphore()
    for device in (partner, after, before, across):
        pl.semaphore_signal(barrier, inc=1, device_id={"tp": device}, device_id_type=MESH)
    fetch.wait()
    total = jnp.zeros((128, 128), f32)
    for j in range(tiles):
        wide = x_s[:, j * TILE : (j + 1) * TILE].astype(f32)
        square = wide * wide
        for m in range(0, TILE, 128):
            total = total + square[:, m : m + 128]
    scale = lax.rsqrt(jnp.sum(total, -1, keepdims=True) / x_ref.shape[1] + 1e-6)
    pl.semaphore_wait(barrier, 4)

    def norm(j, _):
        wide = x_s[:, cols(j)].astype(f32)
        held[j, some(own), :] = (wide * scale * gain_ref[cols(j)].astype(f32)).astype(bf16)
        own_to_partner(j).start()
        message(0, j).start()
        return 0

    lax.fori_loop(0, tiles, norm, 0)

    def unit(j, first, into):
        w = ring[some(lax.rem(j, SLOTS) * TILE, TILE), :]
        term = jnp.dot(held[j, first : first + 256, :], w, preferred_element_type=f32)
        acc[into : into + 256, :] = jnp.where(j == 0, 0.0, acc[into : into + 256, :]) + term

    def turned_head(h, into, blocks):
        for half, t_at in enumerate(blocks):
            rows = some(t_at * 128)
            cos, sin = turn_s[rows, :HEAD], turn_s[rows, HEAD:]
            for m in range(3):
                t = acc[into + half * 128 : into + half * 128 + 128, cols(m * heads + h, HEAD)].astype(bf16)
                if m < 2:
                    t = t.astype(f32)
                    t = (t * cos + pltpu.roll(t, HEAD // 2, 1) * sin).astype(bf16)
                qkv[m * heads + h, rows, :] = t

    def turned_heads(into, blocks):
        lax.fori_loop(0, heads, lambda h, _: turned_head(h, into, blocks), None)

    def arrivals(s):
        p, q = chip_at(chips - 1), chip_at(1)
        p_first, q_first = 2 * lax.rem(p + chips - 1, chips), 2 * lax.rem(q + 1, chips) + 1
        return [(2 * p, 2 * q + 1),
                (jnp.where(p != 0, p_first, 2 * p + 1), jnp.where(q == chips - 1, q_first, 2 * q)),
                (jnp.where(p != 0, 2 * p + 1, p_first), jnp.where(q == chips - 1, 2 * q, q_first))][s]

    def came(s, j):
        message(s, j).wait_recv()
        passed(s, j).start()

    def first_came(j):
        came(0, j)

        @pl.when(early)
        def _():
            message(1, j).start()

    def refill(j, more):
        @pl.when(more)
        def _():
            for copy in weights(lax.rem(j + SLOTS, tiles)):
                copy.start(priority=1)

    def own_chip(j, _):
        own_to_partner(j).wait_recv()

        @pl.when(jnp.logical_not(early))
        def _():
            message(1, j).start()

        @pl.when(j >= 3)
        def _():
            first_came(j - 3)

        for copy in weights(j):
            copy.wait()
        unit(j, 0, 0)
        refill(j, True)
        return 0

    lax.fori_loop(0, tiles, own_chip, 0)
    fetch_turn.wait()

    def first_arrivals(j, _):
        @pl.when(j < 3)
        def _():
            first_came(j + tiles - 3)

        message(2, j).start()

        @pl.when(j >= 5)
        def _():
            came(1, j - 5)

        passed(0, j, other).wait_recv()
        for copy in weights(j):
            copy.wait()
        turned_head(j, 0, (2 * chip, 2 * chip + 1))
        unit(j, 256, 256)
        refill(j, True)
        return 0

    lax.fori_loop(0, tiles, first_arrivals, 0)

    def second_arrivals(j, _):
        @pl.when(j + 4 < tiles)
        def _():
            came(1, j + 4)

        passed(1, j, other).wait_recv()
        for copy in weights(j):
            copy.wait()
        turned_head(j, 256, arrivals(0))
        unit(j, 512, 0)
        refill(j, j + SLOTS < tiles)
        return 0

    lax.fori_loop(0, tiles, second_arrivals, 0)
    for i in range(6):
        wo_tile(i).start(priority=1)

    def sent_first(j, _):
        own_to_partner(j).wait_send()
        message(0, j).wait_send()
        passed(1, j).wait_send()
        return 0

    lax.fori_loop(0, tiles, sent_first, 0)
    for i, device in enumerate((partner, before)):
        pl.semaphore_signal(free.at[i], inc=1, device_id={"tp": device}, device_id_type=MESH)
    turned_heads(0, arrivals(1))

    e = HEAD**-0.5 * LOG2E

    def dot(a, b, ca, cb):
        return lax.dot_general(a, b, (((ca,), (cb,)), ((), ())), preferred_element_type=f32)

    def attention(t, into):
        queries = some(t * 128)

        def block(at, size, seen_before, diagonal):
            keys = some(at, size)
            scores = [dot(qkv[heads + h, keys, :], qkv[h, queries, :], 1, 1) for h in range(heads)]
            weights, keeps = [], []
            for h, s in enumerate(scores):
                if diagonal:
                    key = lax.broadcasted_iota(jnp.int32, (size, 128), 0)
                    s = jnp.where(lax.broadcasted_iota(jnp.int32, (size, 128), 1) + (size - 128) >= key, s, HIDDEN)
                top = s.max(axis=0, keepdims=True)
                if seen_before:
                    old = top_s[h : h + 1, :]
                    top = jnp.maximum(old, top)
                    keeps.append(jnp.exp2((old - top) * e))
                top_s[h : h + 1, :] = top
                weights.append(jnp.exp2((s - top) * e).astype(bf16))
            for h, p in enumerate(weights):
                values = jnp.concatenate([qkv[2 * heads + h, keys, :].T, jnp.ones((8, size), bf16)], axis=0)
                got = dot(values, p, 1, 0)
                mix_s[h] = mix_s[h] * keeps[h] + got if seen_before else got

        @pl.when(t % 2 == 0)
        def _():
            block(t * 128, 128, False, True)

        @pl.when(t % 2 == 1)
        def _():
            block((t - 1) * 128, 256, False, True)

        lax.fori_loop(0, t // 2, lambda j, _: block(j * 256, 256, True, False), None)
        for h in range(heads):
            got = (mix_s[h, :HEAD, :] * (1 / mix_s[h, HEAD : HEAD + 1, :])).T.astype(bf16)
            seen[some(into), h * HEAD : (h + 1) * HEAD] = got

    far, right, left = chip_at(2), chip_at(1), chip_at(chips - 1)
    got_far_first = ((core == 0) & (chip == chips - 1)) | ((core == 1) & (chip != 0))
    into_far = jnp.where(got_far_first, 0, 1)

    def blocks_of(b):
        right_far, left_far = chip == chips // 2, chip != 1
        to_right = pick(b, [jnp.where(right_far, 2 * far + 1, 2 * right), jnp.where(right_far, 2 * right, 2 * far + 1), 2 * chip, 2 * right + 1])
        to_left = pick(b, [jnp.where(left_far, 2 * far, 2 * left + 1), jnp.where(left_far, 2 * left + 1, 2 * far), 2 * chip + 1, 2 * left])
        return jnp.where(core == 0, to_right, to_left), jnp.where(core == 0, to_left, to_right)

    def place(i):
        return pl.ds(pl.multiple_of(i // 3 * 64, 64), 64), cols(lax.rem(i, 3))

    def tile(b, j, i, count):
        wo_tile(i).wait()
        rows, columns = wo_slot(i)
        term = jnp.dot(seen[...], ring[rows, columns], preferred_element_type=f32)

        @pl.when(b > 0)
        def _():
            exchange(b - 1, j).wait_send()

        for half in range(2):
            acc[place(18 + lax.rem(j, 3) * 2 + half)] = term[half * 64 : half * 64 + 64]
        held[j, some(own), :] = term[128:].astype(bf16)
        exchange(b, j).start()

        @pl.when(i + 6 < count)
        def _():
            wo_tile(i + 6).start(priority=1)

    def finish(b, j):
        exchange(b, j).wait_recv()
        got = held[j, exchanged(b), :].astype(f32)
        low = acc[place(18 + lax.rem(j, 3) * 2)] + got[:64]
        high = acc[place(18 + lax.rem(j, 3) * 2 + 1)] + got[64:]

        @pl.when(b < 2)
        def _():
            at = pl.multiple_of(jnp.where(b == 0, EXCHANGED[0], EXCHANGED[1]), 128)
            held[j, pl.ds(at, 64), :] = low.astype(bf16)
            held[j, pl.ds(at + 64, 64), :] = high.astype(bf16)

        for kind in range(2):

            @pl.when(b == kind)
            def _():
                onwards(kind, j).start()

        @pl.when(b == 2)
        def _():
            acc[place(2 * j)] = low
            acc[place(2 * j + 1)] = high

        @pl.when(b == 3)
        def _():
            arrival(into_far, j).wait_recv()
            more = held[j, some(pick(into_far, INTO)), :].astype(f32)
            at = EXCHANGED[3]
            held[j, at : at + 64, :] = (low + more[:64]).astype(bf16)
            held[j, at + 64 : at + 128, :] = (high + more[64:]).astype(bf16)
            onwards(2, j).start()

    def attend(b):
        mine, others = blocks_of(b)

        def one(i, _):
            attention(jnp.where(i == 0, mine, others), i * 128)
            return 0

        lax.fori_loop(0, 2, one, 0)

    def first_step(b, _):
        attend(b)
        for i in range(2):
            pl.semaphore_wait(free.at[i], 1)

        def step(j, _):
            @pl.when(j < tiles)
            def _():
                tile(b, j, j, tiles)

            @pl.when(j >= LAG)
            def _():
                finish(b, j - LAG)

            @pl.when(j < tiles)
            def _():
                came(2, j)

            return 0

        lax.fori_loop(0, tiles + LAG, step, 0)
        return 0

    lax.fori_loop(0, 1, first_step, 0)
    for j in range(SLOTS):
        for copy in weights(j):
            copy.start(priority=1)

    def last_arrivals(j, _):
        passed(2, j, other).wait_recv()
        for copy in weights(j):
            copy.wait()
        unit(j, 768, 0)
        refill(j, j + SLOTS < tiles)
        return 0

    lax.fori_loop(0, tiles, last_arrivals, 0)
    for i in range(6):
        wo_tile(i).start(priority=1)

    def sent(j, _):
        for s in (1, 2):
            message(s, j).wait_send()
        for s in (0, 2):
            passed(s, j).wait_send()
        return 0

    lax.fori_loop(0, tiles, sent, 0)
    for i, device in enumerate((partner, before, across)):
        pl.semaphore_signal(free.at[2 + i], inc=1, device_id={"tp": device}, device_id_type=MESH)
    turned_heads(0, arrivals(2))

    def later_step(b, _):
        attend(b)

        @pl.when(b == 1)
        def _():
            for i in range(3):
                pl.semaphore_wait(free.at[2 + i], 1)

        def step(j, _):
            @pl.when(j < tiles)
            def _():
                tile(b, j, (b - 1) * tiles + j, 3 * tiles)

            @pl.when(j >= LAG)
            def _():
                finish(b, j - LAG)

            return 0

        lax.fori_loop(0, tiles + LAG, step, 0)
        return 0

    lax.fori_loop(1, 4, later_step, 0)

    def last(j, _):
        exchange(3, j).wait_send()
        arrival(1 - into_far, j).wait_recv()
        arrival(2, j).wait_recv()
        near = held[j, some(pick(1 - into_far, INTO)), :].astype(f32)
        for half in range(2):
            rows = slice(half * 64, half * 64 + 64)
            total = acc[place(2 * j + half)] + near[rows] + held[j, INTO[2] + half * 64 : INTO[2] + half * 64 + 64, :].astype(f32)
            held[j, pl.ds(pl.multiple_of(own + half * 64, 64), 64), :] = (x_s[rows, cols(j)].astype(f32) + total).astype(bf16)
        out(j).start()
        return 0

    lax.fori_loop(0, tiles, last, 0)

    def done(j, _):
        for kind in range(3):
            onwards(kind, j).wait_send()
        out(j).wait()
        return 0

    lax.fori_loop(0, tiles, done, 0)


def solution(mesh):
    n = mesh.shape["tp"]

    def step(x, gain, wq, wk, wv, wo):
        mine, depth = x.shape
        width = wq.shape[1]
        heads, tiles, rows = width // HEAD, depth // TILE, mine * n
        anywhere = pl.BlockSpec(memory_space=pl.ANY)
        dma = pltpu.SemaphoreType.DMA
        return pl.pallas_call(
            functools.partial(kernel, n),
            out_shape=jax.ShapeDtypeStruct((mine, depth), bf16),
            in_specs=[anywhere, pl.BlockSpec(memory_space=pltpu.VMEM)] + [anywhere] * 5,
            out_specs=anywhere,
            scratch_shapes=[
                pltpu.VMEM((mine, depth), bf16),
                pltpu.VMEM((rows, 2 * HEAD), f32),
                pltpu.VMEM((tiles, rows, TILE), bf16),
                pltpu.VMEM((SLOTS * TILE, 3 * width), bf16),
                pltpu.VMEM((512, 3 * width), f32),
                pltpu.VMEM((3 * heads, rows, HEAD), bf16),
                pltpu.VMEM((256, width), bf16),
                pltpu.VMEM((16, HEAD), f32),
                pltpu.VMEM((heads, HEAD + 8, 128), f32),
                dma((2,)), dma((SLOTS, 3)), dma((6,)), dma((tiles,)),
                dma((tiles,)), dma((tiles,)), dma((3, tiles)), dma((3, tiles)), dma((3, tiles)), dma((3, tiles)),
                dma((4, tiles)), dma((4, tiles)), dma((3, tiles)), dma((3, tiles)),
                pltpu.SemaphoreType.REGULAR((5,)),
            ],
            compiler_params=pltpu.CompilerParams(collective_id=0, has_side_effects=True, vmem_limit_bytes=VMEM),
        )(x, gain, jnp.asarray(rotation(rows)), wq, wk, wv, wo)

    tokens, columns = P(("dp", "tp"), None), P(None, "tp")
    return jax.shard_map(
        step,
        mesh=mesh,
        in_specs=(tokens, P(None), columns, columns, columns, P("tp", None)),
        out_specs=tokens,
        check_vma=False,
    )
```

```python
import functools

import jax
import jax.numpy as jnp
import numpy as np
from jax import lax
from jax.experimental import pallas as pl
from jax.experimental.pallas import tpu as pltpu
from jax.sharding import PartitionSpec as P

HEAD = 128
THETA = 10000
LOG2E = 1.4426950408889634
HIDDEN = -2e30
VMEM = 63 * 2**20
CORES = 2
TILE = 1024
SLOTS = 3
LAG = 2
MESH = pl.DeviceIdType.MESH
f32, bf16 = jnp.float32, jnp.bfloat16

INTO = (640, 256, 384)
EXCHANGED = (512, 768, 896, None)


def rotation(rows):
    half = HEAD // 2
    angle = np.arange(rows, dtype=np.float64)[:, None] * float(THETA) ** (-np.arange(half, dtype=np.float64) / half)
    cos, sin = np.cos(angle), np.sin(angle)
    return np.concatenate([cos, cos, -sin, sin], 1).astype(np.float32)


def pick(i, values):
    got = values[-1]
    for m in range(len(values) - 2, -1, -1):
        got = jnp.where(i == m, values[m], got)
    return got


def kernel(n, x_ref, gain_ref, turn_ref, wq_ref, wk_ref, wv_ref, wo_ref, y_ref,
           x_s, turn_s, held, ring, acc, qkv, seen, top_s, mix_s,
           in_sem, w_sem, wo_sem, y_sem, own_send, own_recv, to_send, to_recv, pass_send, pass_recv, ex_send, ex_recv, rs_send, rs_recv, free):
    me = lax.axis_index("tp")
    chips = n // CORES
    chip, core = me // CORES, me % CORES
    chip_at = lambda ahead: lax.rem(chip + ahead, chips)
    partner = chip * CORES + 1 - core
    forth, back = jnp.where(core == 0, 1, chips - 1), jnp.where(core == 0, chips - 1, 1)
    after, before = chip_at(forth) * CORES + core, chip_at(back) * CORES + core
    across = chip_at(forth) * CORES + 1 - core
    own = pl.multiple_of(core * 128, 128)
    other = pl.multiple_of((1 - core) * 128, 128)
    tiles = x_ref.shape[1] // TILE
    width = wq_ref.shape[1]
    heads = width // HEAD
    early = ((core == 0) & (chip != 0)) | ((core == 1) & (chip == chips - 1))

    def cols(j, size=TILE):
        return pl.ds(pl.multiple_of(j * size, 128), size)

    def some(r, size=128):
        return pl.ds(pl.multiple_of(r, 128), size)

    def weights(j):
        slot = lax.rem(j, SLOTS)
        return [pltpu.make_async_copy(w.at[cols(j), :], ring.at[some(slot * TILE, TILE), pl.ds(m * width, width)], w_sem.at[slot, m])
                for m, w in enumerate((wq_ref, wk_ref, wv_ref))]

    def wo_slot(i, depth):
        slot = lax.rem(i, depth)
        return some(slot // 3 * width, width), cols(lax.rem(slot, 3))

    def wo_tile(i, depth):
        rows, columns = wo_slot(i, depth)
        return pltpu.make_async_copy(wo_ref.at[:, cols(lax.rem(i, tiles))], ring.at[rows, columns], wo_sem.at[lax.rem(i, depth)])

    def remote(j, at, to, send, recv, device):
        return pltpu.make_async_remote_copy(src_ref=held.at[j, some(at), :], dst_ref=held.at[j, some(to), :], send_sem=send, recv_sem=recv,
                                            device_id={"tp": device}, device_id_type=MESH)

    def own_to_partner(j):
        return remote(j, own, own, own_send.at[j], own_recv.at[j], partner)

    def message(s, j):
        first = 256 + own
        at = (own, jnp.where(early, first, other), jnp.where(early, other, first))[s]
        return remote(j, at, 256 + s * 256 + own, to_send.at[s, j], to_recv.at[s, j], after)

    def passed(s, j, core_at=own):
        return remote(j, 256 + s * 256 + core_at, 256 + s * 256 + core_at, pass_send.at[s, j], pass_recv.at[s, j], partner)

    def exchange(b, j):
        return remote(j, own, pick(b, [own if r is None else r for r in EXCHANGED]), ex_send.at[b, j], ex_recv.at[b, j], partner)

    def exchanged(b):
        return some(pick(b, [other if r is None else r for r in EXCHANGED]))

    def onwards(kind, j):
        at = EXCHANGED[kind]
        return remote(j, at, INTO[kind], rs_send.at[kind, j], rs_recv.at[kind, j], after if kind < 2 else across)

    def arrival(kind, j):
        return remote(j, EXCHANGED[0], pick(kind, INTO), rs_send.at[kind, j], rs_recv.at[kind, j], after)

    def out(j):
        return pltpu.make_async_copy(held.at[j, some(own), :], y_ref.at[:, cols(j)], y_sem.at[j])

    fetch = pltpu.make_async_copy(x_ref, x_s, in_sem.at[0])
    fetch.start()
    for j in range(SLOTS):
        for copy in weights(j):
            copy.start(priority=1)
    fetch_turn = pltpu.make_async_copy(turn_ref, turn_s, in_sem.at[1])
    fetch_turn.start()
    barrier = pltpu.get_barrier_semaphore()
    for device in (partner, after, before, across):
        pl.semaphore_signal(barrier, inc=1, device_id={"tp": device}, device_id_type=MESH)
    fetch.wait()
    total = jnp.zeros((128, 128), f32)
    for j in range(tiles):
        wide = x_s[:, j * TILE : (j + 1) * TILE].astype(f32)
        square = wide * wide
        for m in range(0, TILE, 128):
            total = total + square[:, m : m + 128]
    scale = lax.rsqrt(jnp.sum(total, -1, keepdims=True) / x_ref.shape[1] + 1e-6)

    def norm(j, _):
        wide = x_s[:, cols(j)].astype(f32)
        held[j, some(own), :] = (wide * scale * gain_ref[cols(j)].astype(f32)).astype(bf16)
        return 0

    lax.fori_loop(0, tiles, norm, 0)
    pl.semaphore_wait(barrier, 4)

    def send(j, _):
        own_to_partner(j).start()
        message(0, j).start()
        return 0

    lax.fori_loop(0, tiles, send, 0)

    def unit(j, first, into, fresh):
        w = ring[some(lax.rem(j, SLOTS) * TILE, TILE), :]
        term = jnp.dot(held[j, first : first + 256, :], w, preferred_element_type=f32)
        acc[into : into + 256, :] = jnp.where(fresh, 0.0, acc[into : into + 256, :]) + term

    def turned_head(h, into, blocks):
        for half, t_at in enumerate(blocks):
            rows = some(t_at * 128)
            cos, sin = turn_s[rows, :HEAD], turn_s[rows, HEAD:]
            for m in range(3):
                t = acc[into + half * 128 : into + half * 128 + 128, cols(m * heads + h, HEAD)].astype(bf16)
                if m < 2:
                    t = t.astype(f32)
                    t = (t * cos + pltpu.roll(t, HEAD // 2, 1) * sin).astype(bf16)
                qkv[m * heads + h, rows, :] = t

    def turned_heads(into, blocks):
        lax.fori_loop(0, heads, lambda h, _: turned_head(h, into, blocks), None)

    def arrivals(s):
        p, q = chip_at(chips - 1), chip_at(1)
        p_first, q_first = 2 * lax.rem(p + chips - 1, chips), 2 * lax.rem(q + 1, chips) + 1
        return [(2 * p, 2 * q + 1),
                (jnp.where(p != 0, p_first, 2 * p + 1), jnp.where(q == chips - 1, q_first, 2 * q)),
                (jnp.where(p != 0, 2 * p + 1, p_first), jnp.where(q == chips - 1, 2 * q, q_first))][s]

    def came(s, j):
        message(s, j).wait_recv()
        passed(s, j).start()

    def first_came(j):
        came(0, j)

        @pl.when(early)
        def _():
            message(1, j).start()

    def refill(j, more):
        @pl.when(more)
        def _():
            for copy in weights(lax.rem(j + SLOTS, tiles)):
                copy.start(priority=1)

    def own_chip(j, _):
        own_to_partner(j).wait_recv()

        @pl.when(jnp.logical_not(early))
        def _():
            message(1, j).start()

        @pl.when(j >= 3)
        def _():
            first_came(j - 3)

        for copy in weights(j):
            copy.wait()
        unit(j, 0, 0, j == 0)
        refill(j, True)
        return 0

    lax.fori_loop(0, tiles, own_chip, 0)
    fetch_turn.wait()

    def first_arrivals(j, _):
        @pl.when(j < 3)
        def _():
            first_came(j + tiles - 3)

        message(2, j).start()

        @pl.when(j >= 4)
        def _():
            came(1, j - 4)

        passed(0, j, other).wait_recv()
        for copy in weights(j):
            copy.wait()
        turned_head(j, 0, (2 * chip, 2 * chip + 1))
        unit(j, 256, 256, j == 0)
        refill(j, True)
        return 0

    lax.fori_loop(0, tiles, first_arrivals, 0)

    def second_arrivals(j, _):
        @pl.when((j >= 3) & (j + 2 < tiles))
        def _():
            came(1, j + 2)

        passed(1, j, other).wait_recv()
        for copy in weights(j):
            copy.wait()
        turned_head(j, 256, arrivals(0))
        unit(j, 512, 0, j == 0)
        refill(j, j + SLOTS < tiles)
        return 0

    lax.fori_loop(0, tiles, second_arrivals, 0)
    for i in range(3):
        wo_tile(i, 3).start(priority=1)
    for copy in weights(2):
        copy.start(priority=1)

    def sent_first(j, _):
        own_to_partner(j).wait_send()
        message(0, j).wait_send()
        passed(1, j).wait_send()
        return 0

    lax.fori_loop(0, tiles, sent_first, 0)
    for i, device in enumerate((partner, before)):
        pl.semaphore_signal(free.at[i], inc=1, device_id={"tp": device}, device_id_type=MESH)
    turned_heads(0, arrivals(1))

    e = HEAD**-0.5 * LOG2E

    def dot(a, b, ca, cb):
        return lax.dot_general(a, b, (((ca,), (cb,)), ((), ())), preferred_element_type=f32)

    def attention(t, into):
        queries = some(t * 128)

        def block(at, size, seen_before, diagonal):
            keys = some(at, size)
            scores = [dot(qkv[heads + h, keys, :], qkv[h, queries, :], 1, 1) for h in range(heads)]
            weights, keeps = [], []
            for h, s in enumerate(scores):
                if diagonal:
                    key = lax.broadcasted_iota(jnp.int32, (size, 128), 0)
                    s = jnp.where(lax.broadcasted_iota(jnp.int32, (size, 128), 1) + (size - 128) >= key, s, HIDDEN)
                top = s.max(axis=0, keepdims=True)
                if seen_before:
                    old = top_s[h : h + 1, :]
                    top = jnp.maximum(old, top)
                    keeps.append(jnp.exp2((old - top) * e))
                top_s[h : h + 1, :] = top
                weights.append(jnp.exp2((s - top) * e).astype(bf16))
            for h, p in enumerate(weights):
                values = jnp.concatenate([qkv[2 * heads + h, keys, :].T, jnp.ones((8, size), bf16)], axis=0)
                got = dot(values, p, 1, 0)
                mix_s[h] = mix_s[h] * keeps[h] + got if seen_before else got

        @pl.when(t % 2 == 0)
        def _():
            block(t * 128, 128, False, True)

        @pl.when(t % 2 == 1)
        def _():
            block((t - 1) * 128, 256, False, True)

        lax.fori_loop(0, t // 2, lambda j, _: block(j * 256, 256, True, False), None)
        for h in range(heads):
            got = (mix_s[h, :HEAD, :] * (1 / mix_s[h, HEAD : HEAD + 1, :])).T.astype(bf16)
            seen[some(into), h * HEAD : (h + 1) * HEAD] = got

    far, right, left = chip_at(2), chip_at(1), chip_at(chips - 1)
    got_far_first = ((core == 0) & (chip == chips - 1)) | ((core == 1) & (chip != 0))
    into_far = jnp.where(got_far_first, 0, 1)

    def blocks_of(b):
        right_far, left_far = chip == chips // 2, chip != 1
        to_right = pick(b, [jnp.where(right_far, 2 * far + 1, 2 * right), jnp.where(right_far, 2 * right, 2 * far + 1), 2 * right + 1, 2 * chip])
        to_left = pick(b, [jnp.where(left_far, 2 * far, 2 * left + 1), jnp.where(left_far, 2 * left + 1, 2 * far), 2 * left, 2 * chip + 1])
        return jnp.where(core == 0, to_right, to_left), jnp.where(core == 0, to_left, to_right)

    def place(i):
        return pl.ds(pl.multiple_of(i // 3 * 64, 64), 64), cols(lax.rem(i, 3))

    def tile(b, j, i, count, depth):
        wo_tile(i, depth).wait()
        rows, columns = wo_slot(i, depth)
        term = jnp.dot(seen[...], ring[rows, columns], preferred_element_type=f32)

        @pl.when(b > 0)
        def _():
            exchange(b - 1, j).wait_send()

        for half in range(2):
            acc[place(18 + lax.rem(j, 3) * 2 + half)] = term[half * 64 : half * 64 + 64]
        held[j, some(own), :] = term[128:].astype(bf16)
        exchange(b, j).start()

        @pl.when(i + depth < count)
        def _():
            wo_tile(i + depth, depth).start(priority=1)

    def finish(b, j):
        exchange(b, j).wait_recv()
        got = held[j, exchanged(b), :].astype(f32)
        low = acc[place(18 + lax.rem(j, 3) * 2)] + got[:64]
        high = acc[place(18 + lax.rem(j, 3) * 2 + 1)] + got[64:]

        @pl.when(b < 2)
        def _():
            at = pl.multiple_of(jnp.where(b == 0, EXCHANGED[0], EXCHANGED[1]), 128)
            held[j, pl.ds(at, 64), :] = low.astype(bf16)
            held[j, pl.ds(at + 64, 64), :] = high.astype(bf16)

        for kind in range(2):

            @pl.when(b == kind)
            def _():
                onwards(kind, j).start()

        @pl.when(b == 3)
        def _():
            acc[place(2 * j)] = low
            acc[place(2 * j + 1)] = high

        @pl.when(b == 2)
        def _():
            arrival(into_far, j).wait_recv()
            more = held[j, some(pick(into_far, INTO)), :].astype(f32)
            at = EXCHANGED[2]
            held[j, at : at + 64, :] = (low + more[:64]).astype(bf16)
            held[j, at + 64 : at + 128, :] = (high + more[64:]).astype(bf16)
            onwards(2, j).start()

    def attend(b):
        mine, others = blocks_of(b)

        def one(i, _):
            attention(jnp.where(i == 0, mine, others), i * 128)
            return 0

        lax.fori_loop(0, 2, one, 0)

    def first_step(b, _):
        attend(b)
        for i in range(2):
            pl.semaphore_wait(free.at[i], 1)

        def step(j, _):
            @pl.when(j < tiles)
            def _():
                tile(b, j, j, tiles, 3)

            @pl.when(j >= LAG)
            def _():
                finish(b, j - LAG)

            @pl.when((j >= 3) & (j < tiles))
            def _():
                came(2, j - 3)

            return 0

        lax.fori_loop(0, tiles + LAG, step, 0)
        return 0

    lax.fori_loop(0, 1, first_step, 0)
    for j in (3, 4):
        for copy in weights(j):
            copy.start(priority=1)

    def last_arrivals(i, _):
        j = lax.rem(i + 2, tiles)

        @pl.when(i < 3)
        def _():
            came(2, i + tiles - 3)

        passed(2, j, other).wait_recv()
        for copy in weights(j):
            copy.wait()
        unit(j, 768, 0, i == 0)
        refill(j, i + SLOTS < tiles)
        return 0

    lax.fori_loop(0, tiles, last_arrivals, 0)
    for i in range(6):
        wo_tile(i, 6).start(priority=1)

    def sent(j, _):
        for s in (1, 2):
            message(s, j).wait_send()
        for s in (0, 2):
            passed(s, j).wait_send()
        return 0

    lax.fori_loop(0, tiles, sent, 0)
    for i, device in enumerate((partner, before, across)):
        pl.semaphore_signal(free.at[2 + i], inc=1, device_id={"tp": device}, device_id_type=MESH)
    turned_heads(0, arrivals(2))

    def later_step(b, _):
        attend(b)

        @pl.when(b == 1)
        def _():
            for i in range(3):
                pl.semaphore_wait(free.at[2 + i], 1)

        def step(j, _):
            @pl.when(j < tiles)
            def _():
                tile(b, j, (b - 1) * tiles + j, 3 * tiles, 6)

            @pl.when(j >= LAG)
            def _():
                finish(b, j - LAG)

            return 0

        lax.fori_loop(0, tiles + LAG, step, 0)
        return 0

    lax.fori_loop(1, 4, later_step, 0)

    def last(j, _):
        exchange(3, j).wait_send()
        arrival(1 - into_far, j).wait_recv()
        arrival(2, j).wait_recv()
        near = held[j, some(pick(1 - into_far, INTO)), :].astype(f32)
        for half in range(2):
            rows = slice(half * 64, half * 64 + 64)
            total = acc[place(2 * j + half)] + near[rows] + held[j, INTO[2] + half * 64 : INTO[2] + half * 64 + 64, :].astype(f32)
            held[j, pl.ds(pl.multiple_of(own + half * 64, 64), 64), :] = (x_s[rows, cols(j)].astype(f32) + total).astype(bf16)
        out(j).start()
        return 0

    lax.fori_loop(0, tiles, last, 0)

    def done(j, _):
        for kind in range(3):
            onwards(kind, j).wait_send()
        out(j).wait()
        return 0

    lax.fori_loop(0, tiles, done, 0)


def solution(mesh):
    n = mesh.shape["tp"]

    def step(x, gain, wq, wk, wv, wo):
        mine, depth = x.shape
        width = wq.shape[1]
        heads, tiles, rows = width // HEAD, depth // TILE, mine * n
        anywhere = pl.BlockSpec(memory_space=pl.ANY)
        dma = pltpu.SemaphoreType.DMA
        return pl.pallas_call(
            functools.partial(kernel, n),
            out_shape=jax.ShapeDtypeStruct((mine, depth), bf16),
            in_specs=[anywhere, pl.BlockSpec(memory_space=pltpu.VMEM)] + [anywhere] * 5,
            out_specs=anywhere,
            scratch_shapes=[
                pltpu.VMEM((mine, depth), bf16),
                pltpu.VMEM((rows, 2 * HEAD), f32),
                pltpu.VMEM((tiles, rows, TILE), bf16),
                pltpu.VMEM((SLOTS * TILE, 3 * width), bf16),
                pltpu.VMEM((512, 3 * width), f32),
                pltpu.VMEM((3 * heads, rows, HEAD), bf16),
                pltpu.VMEM((256, width), bf16),
                pltpu.VMEM((16, HEAD), f32),
                pltpu.VMEM((heads, HEAD + 8, 128), f32),
                dma((2,)), dma((SLOTS, 3)), dma((6,)), dma((tiles,)),
                dma((tiles,)), dma((tiles,)), dma((3, tiles)), dma((3, tiles)), dma((3, tiles)), dma((3, tiles)),
                dma((4, tiles)), dma((4, tiles)), dma((3, tiles)), dma((3, tiles)),
                pltpu.SemaphoreType.REGULAR((5,)),
            ],
            compiler_params=pltpu.CompilerParams(collective_id=0, has_side_effects=True, vmem_limit_bytes=VMEM),
        )(x, gain, jnp.asarray(rotation(rows)), wq, wk, wv, wo)

    tokens, columns = P(("dp", "tp"), None), P(None, "tp")
    return jax.shard_map(
        step,
        mesh=mesh,
        in_specs=(tokens, P(None), columns, columns, columns, P("tp", None)),
        out_specs=tokens,
        check_vma=False,
    )
```

```python
import functools

import jax
import jax.numpy as jnp
import numpy as np
from jax import lax
from jax.experimental import pallas as pl
from jax.experimental.pallas import tpu as pltpu
from jax.sharding import PartitionSpec as P

HEAD = 128
THETA = 10000
LOG2E = 1.4426950408889634
HIDDEN = -2e30
VMEM = 63 * 2**20
CORES = 2
TILE = 1024
SLOTS = 3
LAG = 3
MESH = pl.DeviceIdType.MESH
f32, bf16 = jnp.float32, jnp.bfloat16

INTO = (640, 256, 384)
EXCHANGED = (512, 768, 896, None)


def rotation(rows):
    half = HEAD // 2
    angle = np.arange(rows, dtype=np.float64)[:, None] * float(THETA) ** (-np.arange(half, dtype=np.float64) / half)
    cos, sin = np.cos(angle), np.sin(angle)
    return np.concatenate([cos, cos, -sin, sin], 1).astype(np.float32)


def pick(i, values):
    got = values[-1]
    for m in range(len(values) - 2, -1, -1):
        got = jnp.where(i == m, values[m], got)
    return got


def kernel(n, x_ref, gain_ref, turn_ref, wq_ref, wk_ref, wv_ref, wo_ref, y_ref,
           x_s, turn_s, held, ring, acc, qkv, seen, top_s, mix_s,
           in_sem, w_sem, wo_sem, y_sem, own_send, own_recv, to_send, to_recv, pass_send, pass_recv, ex_send, ex_recv, rs_send, rs_recv, free):
    me = lax.axis_index("tp")
    chips = n // CORES
    chip, core = me // CORES, me % CORES
    chip_at = lambda ahead: lax.rem(chip + ahead, chips)
    partner = chip * CORES + 1 - core
    forth, back = jnp.where(core == 0, 1, chips - 1), jnp.where(core == 0, chips - 1, 1)
    after, before = chip_at(forth) * CORES + core, chip_at(back) * CORES + core
    across = chip_at(forth) * CORES + 1 - core
    own = pl.multiple_of(core * 128, 128)
    other = pl.multiple_of((1 - core) * 128, 128)
    tiles = x_ref.shape[1] // TILE
    width = wq_ref.shape[1]
    heads = width // HEAD
    early = ((core == 0) & (chip != 0)) | ((core == 1) & (chip == chips - 1))

    def cols(j, size=TILE):
        return pl.ds(pl.multiple_of(j * size, 128), size)

    def some(r, size=128):
        return pl.ds(pl.multiple_of(r, 128), size)

    def weights(j):
        slot = lax.rem(j, SLOTS)
        return [pltpu.make_async_copy(w.at[cols(j), :], ring.at[some(slot * TILE, TILE), pl.ds(m * width, width)], w_sem.at[slot, m])
                for m, w in enumerate((wq_ref, wk_ref, wv_ref))]

    def wo_slot(i, depth):
        slot = lax.rem(i, depth)
        return some(slot // 3 * width, width), cols(lax.rem(slot, 3))

    def wo_tile(i, depth):
        rows, columns = wo_slot(i, depth)
        return pltpu.make_async_copy(wo_ref.at[:, cols(lax.rem(i, tiles))], ring.at[rows, columns], wo_sem.at[lax.rem(i, depth)])

    def remote(j, at, to, send, recv, device):
        return pltpu.make_async_remote_copy(src_ref=held.at[j, some(at), :], dst_ref=held.at[j, some(to), :], send_sem=send, recv_sem=recv,
                                            device_id={"tp": device}, device_id_type=MESH)

    def own_to_partner(j):
        return remote(j, own, own, own_send.at[j], own_recv.at[j], partner)

    def message(s, j):
        first = 256 + own
        at = (own, jnp.where(early, first, other), jnp.where(early, other, first))[s]
        return remote(j, at, 256 + s * 256 + own, to_send.at[s, j], to_recv.at[s, j], after)

    def passed(s, j, core_at=own):
        return remote(j, 256 + s * 256 + core_at, 256 + s * 256 + core_at, pass_send.at[s, j], pass_recv.at[s, j], partner)

    def exchange(b, j):
        return remote(j, own, pick(b, [own if r is None else r for r in EXCHANGED]), ex_send.at[b, j], ex_recv.at[b, j], partner)

    def exchanged(b):
        return some(pick(b, [other if r is None else r for r in EXCHANGED]))

    def onwards(kind, j):
        at = EXCHANGED[kind]
        return remote(j, at, INTO[kind], rs_send.at[kind, j], rs_recv.at[kind, j], after if kind < 2 else across)

    def arrival(kind, j):
        return remote(j, EXCHANGED[0], pick(kind, INTO), rs_send.at[kind, j], rs_recv.at[kind, j], after)

    def out(j):
        return pltpu.make_async_copy(held.at[j, some(own), :], y_ref.at[:, cols(j)], y_sem.at[j])

    fetch = pltpu.make_async_copy(x_ref, x_s, in_sem.at[0])
    fetch.start()
    for j in range(SLOTS):
        for copy in weights(j):
            copy.start(priority=1)
    fetch_turn = pltpu.make_async_copy(turn_ref, turn_s, in_sem.at[1])
    fetch_turn.start()
    barrier = pltpu.get_barrier_semaphore()
    for device in (partner, after, before, across):
        pl.semaphore_signal(barrier, inc=1, device_id={"tp": device}, device_id_type=MESH)
    fetch.wait()
    total = jnp.zeros((128, 128), f32)
    for j in range(tiles):
        wide = x_s[:, j * TILE : (j + 1) * TILE].astype(f32)
        square = wide * wide
        for m in range(0, TILE, 128):
            total = total + square[:, m : m + 128]
    scale = lax.rsqrt(jnp.sum(total, -1, keepdims=True) / x_ref.shape[1] + 1e-6)

    def norm(j, _):
        wide = x_s[:, cols(j)].astype(f32)
        held[j, some(own), :] = (wide * scale * gain_ref[cols(j)].astype(f32)).astype(bf16)
        return 0

    lax.fori_loop(0, tiles, norm, 0)
    pl.semaphore_wait(barrier, 4)

    def send(j, _):
        own_to_partner(j).start()
        message(0, j).start()
        return 0

    lax.fori_loop(0, tiles, send, 0)

    def unit(j, first, into, fresh):
        w = ring[some(lax.rem(j, SLOTS) * TILE, TILE), :]
        term = jnp.dot(held[j, first : first + 256, :], w, preferred_element_type=f32)
        acc[into : into + 256, :] = jnp.where(fresh, 0.0, acc[into : into + 256, :]) + term

    def turned_head(h, into, blocks):
        for half, t_at in enumerate(blocks):
            rows = some(t_at * 128)
            cos, sin = turn_s[rows, :HEAD], turn_s[rows, HEAD:]
            for m in range(3):
                t = acc[into + half * 128 : into + half * 128 + 128, cols(m * heads + h, HEAD)].astype(bf16)
                if m < 2:
                    t = t.astype(f32)
                    t = (t * cos + pltpu.roll(t, HEAD // 2, 1) * sin).astype(bf16)
                qkv[m * heads + h, rows, :] = t

    def turned_heads(into, blocks):
        lax.fori_loop(0, heads, lambda h, _: turned_head(h, into, blocks), None)

    def arrivals(s):
        p, q = chip_at(chips - 1), chip_at(1)
        p_first, q_first = 2 * lax.rem(p + chips - 1, chips), 2 * lax.rem(q + 1, chips) + 1
        return [(2 * p, 2 * q + 1),
                (jnp.where(p != 0, p_first, 2 * p + 1), jnp.where(q == chips - 1, q_first, 2 * q)),
                (jnp.where(p != 0, 2 * p + 1, p_first), jnp.where(q == chips - 1, 2 * q, q_first))][s]

    def came(s, j):
        message(s, j).wait_recv()
        passed(s, j).start()

    def first_came(j):
        came(0, j)

        @pl.when(early)
        def _():
            message(1, j).start()

    def refill(j, more):
        @pl.when(more)
        def _():
            for copy in weights(lax.rem(j + SLOTS, tiles)):
                copy.start(priority=1)

    def own_chip(j, _):
        own_to_partner(j).wait_recv()

        @pl.when(jnp.logical_not(early))
        def _():
            message(1, j).start()

        @pl.when(j >= 3)
        def _():
            first_came(j - 3)

        for copy in weights(j):
            copy.wait()
        unit(j, 0, 0, j == 0)
        refill(j, True)
        return 0

    lax.fori_loop(0, tiles, own_chip, 0)
    fetch_turn.wait()

    def first_arrivals(j, _):
        @pl.when(j < 3)
        def _():
            first_came(j + tiles - 3)

        message(2, j).start()

        @pl.when(j >= 5)
        def _():
            came(1, j - 5)

        passed(0, j, other).wait_recv()
        for copy in weights(j):
            copy.wait()
        turned_head(j, 0, (2 * chip, 2 * chip + 1))
        unit(j, 256, 256, j == 0)
        refill(j, True)
        return 0

    lax.fori_loop(0, tiles, first_arrivals, 0)

    def second_arrivals(j, _):
        @pl.when((j >= 3) & (j + 1 < tiles))
        def _():
            came(1, j + 1)

        passed(1, j, other).wait_recv()
        for copy in weights(j):
            copy.wait()
        turned_head(j, 256, arrivals(0))
        unit(j, 512, 0, j == 0)
        refill(j, j + SLOTS < tiles)
        return 0

    lax.fori_loop(0, tiles, second_arrivals, 0)
    for i in range(3):
        wo_tile(i, 3).start(priority=1)
    for copy in weights(2):
        copy.start(priority=1)

    def sent_first(j, _):
        own_to_partner(j).wait_send()
        message(0, j).wait_send()
        passed(1, j).wait_send()
        return 0

    lax.fori_loop(0, tiles, sent_first, 0)
    for i, device in enumerate((partner, before)):
        pl.semaphore_signal(free.at[i], inc=1, device_id={"tp": device}, device_id_type=MESH)
    turned_heads(0, arrivals(1))

    e = HEAD**-0.5 * LOG2E

    def dot(a, b, ca, cb):
        return lax.dot_general(a, b, (((ca,), (cb,)), ((), ())), preferred_element_type=f32)

    def attention(t, into):
        queries = some(t * 128)

        def block(at, size, seen_before, diagonal):
            keys = some(at, size)
            scores = [dot(qkv[heads + h, keys, :], qkv[h, queries, :], 1, 1) for h in range(heads)]
            weights, keeps = [], []
            for h, s in enumerate(scores):
                if diagonal:
                    key = lax.broadcasted_iota(jnp.int32, (size, 128), 0)
                    s = jnp.where(lax.broadcasted_iota(jnp.int32, (size, 128), 1) + (size - 128) >= key, s, HIDDEN)
                top = s.max(axis=0, keepdims=True)
                if seen_before:
                    old = top_s[h : h + 1, :]
                    top = jnp.maximum(old, top)
                    keeps.append(jnp.exp2((old - top) * e))
                top_s[h : h + 1, :] = top
                weights.append(jnp.exp2((s - top) * e).astype(bf16))
            for h, p in enumerate(weights):
                values = jnp.concatenate([qkv[2 * heads + h, keys, :].T, jnp.ones((8, size), bf16)], axis=0)
                got = dot(values, p, 1, 0)
                mix_s[h] = mix_s[h] * keeps[h] + got if seen_before else got

        @pl.when(t % 2 == 0)
        def _():
            block(t * 128, 128, False, True)

        @pl.when(t % 2 == 1)
        def _():
            block((t - 1) * 128, 256, False, True)

        lax.fori_loop(0, t // 2, lambda j, _: block(j * 256, 256, True, False), None)
        for h in range(heads):
            got = (mix_s[h, :HEAD, :] * (1 / mix_s[h, HEAD : HEAD + 1, :])).T.astype(bf16)
            seen[some(into), h * HEAD : (h + 1) * HEAD] = got

    far, right, left = chip_at(2), chip_at(1), chip_at(chips - 1)
    got_far_first = ((core == 0) & (chip == chips - 1)) | ((core == 1) & (chip != 0))
    into_far = jnp.where(got_far_first, 0, 1)

    def blocks_of(b):
        right_far, left_far = chip == chips // 2, chip != 1
        to_right = pick(b, [jnp.where(right_far, 2 * far + 1, 2 * right), jnp.where(right_far, 2 * right, 2 * far + 1), 2 * right + 1, 2 * chip])
        to_left = pick(b, [jnp.where(left_far, 2 * far, 2 * left + 1), jnp.where(left_far, 2 * left + 1, 2 * far), 2 * left, 2 * chip + 1])
        return jnp.where(core == 0, to_right, to_left), jnp.where(core == 0, to_left, to_right)

    def place(i):
        return pl.ds(pl.multiple_of(i // 3 * 64, 64), 64), cols(lax.rem(i, 3))

    def wait_tile(b, j, i, depth):
        wo_tile(i, depth).wait()

        @pl.when(b > 0)
        def _():
            exchange(b - 1, j).wait_send()

    def tile(b, j, i, depth):
        rows, columns = wo_slot(i, depth)
        term = jnp.dot(seen[...], ring[rows, columns], preferred_element_type=f32)
        for half in range(2):
            acc[place(18 + lax.rem(j, 3) * 2 + half)] = term[half * 64 : half * 64 + 64]
        held[j, some(own), :] = term[128:].astype(bf16)

    def send_tile(b, j, i, count, depth):
        exchange(b, j).start()

        @pl.when(i + depth < count)
        def _():
            wo_tile(i + depth, depth).start(priority=1)

    def add(b, j):
        at = exchanged(b)
        got = held[j, at, :].astype(f32)
        low = acc[place(18 + lax.rem(j, 3) * 2)] + got[:64]
        high = acc[place(18 + lax.rem(j, 3) * 2 + 1)] + got[64:]
        held[j, at, :] = jnp.concatenate([low, high], 0).astype(bf16)
        if not isinstance(b, int):
            acc[place(2 * j)] = low
            acc[place(2 * j + 1)] = high

    def send_sum(b, j):
        for kind in range(2):

            @pl.when(b == kind)
            def _():
                onwards(kind, j).start()

        @pl.when(b == 2)
        def _():
            arrival(into_far, j).wait_recv()
            more = held[j, some(pick(into_far, INTO)), :].astype(f32)
            at = EXCHANGED[2]
            held[j, at : at + 64, :] = (acc[place(2 * j)] + more[:64]).astype(bf16)
            held[j, at + 64 : at + 128, :] = (acc[place(2 * j + 1)] + more[64:]).astype(bf16)
            onwards(2, j).start()

    def finish(b, j):
        exchange(b, j).wait_recv()
        add(b, j)
        send_sum(b, j)

    def tiles_of(b, first, count, depth, besides):
        def begin(j, _):
            wait_tile(b, j, first + j, depth)
            tile(b, j, first + j, depth)
            send_tile(b, j, first + j, count, depth)
            return 0

        def go_on(j, _):
            wait_tile(b, j, first + j, depth)
            exchange(b, j - LAG).wait_recv()
            add(b, j - LAG)
            tile(b, j, first + j, depth)
            send_tile(b, j, first + j, count, depth)
            send_sum(b, j - LAG)
            besides(j)
            return 0

        lax.fori_loop(0, LAG, begin, 0)
        lax.fori_loop(LAG, tiles, go_on, 0)

    def attend(b):
        mine, others = blocks_of(b)

        def one(i, _):
            attention(jnp.where(i == 0, mine, others), i * 128)
            return 0

        lax.fori_loop(0, 2, one, 0)

    attend(0)
    for i in range(2):
        pl.semaphore_wait(free.at[i], 1)

    def also_came(j):
        @pl.when(j >= 3)
        def _():
            came(2, j - 3)

    tiles_of(0, 0, tiles, 3, also_came)
    for j in (3, 4):
        for copy in weights(j):
            copy.start(priority=1)

    def last_arrivals(i, _):
        j = lax.rem(i + 2, tiles)

        @pl.when(i < 3)
        def _():
            came(2, i + tiles - 3)

        @pl.when(i < LAG)
        def _():
            finish(0, i + tiles - LAG)

        passed(2, j, other).wait_recv()
        for copy in weights(j):
            copy.wait()
        unit(j, 768, 0, i == 0)
        refill(j, i + SLOTS < tiles)
        return 0

    lax.fori_loop(0, tiles, last_arrivals, 0)
    for i in range(6):
        wo_tile(i, 6).start(priority=1)

    def sent(j, _):
        for s in (1, 2):
            message(s, j).wait_send()
        for s in (0, 2):
            passed(s, j).wait_send()
        return 0

    lax.fori_loop(0, tiles, sent, 0)
    for i, device in enumerate((partner, before, across)):
        pl.semaphore_signal(free.at[2 + i], inc=1, device_id={"tp": device}, device_id_type=MESH)
    turned_heads(0, arrivals(2))

    def later_step(b, _):
        attend(b)

        @pl.when(b == 1)
        def _():
            for i in range(3):
                pl.semaphore_wait(free.at[2 + i], 1)

        tiles_of(b, (b - 1) * tiles, 3 * tiles, 6, lambda j: None)
        lax.fori_loop(tiles - LAG, tiles, lambda j, _: finish(b, j), None)
        return 0

    lax.fori_loop(1, 4, later_step, 0)

    def last(j, _):
        exchange(3, j).wait_send()
        arrival(1 - into_far, j).wait_recv()
        arrival(2, j).wait_recv()
        near = held[j, some(pick(1 - into_far, INTO)), :].astype(f32)
        for half in range(2):
            rows = slice(half * 64, half * 64 + 64)
            total = acc[place(2 * j + half)] + near[rows] + held[j, INTO[2] + half * 64 : INTO[2] + half * 64 + 64, :].astype(f32)
            held[j, pl.ds(pl.multiple_of(own + half * 64, 64), 64), :] = (x_s[rows, cols(j)].astype(f32) + total).astype(bf16)
        out(j).start()
        return 0

    lax.fori_loop(0, tiles, last, 0)

    def done(j, _):
        for kind in range(3):
            onwards(kind, j).wait_send()
        out(j).wait()
        return 0

    lax.fori_loop(0, tiles, done, 0)


def handed_on(from_ref, to_ref, room, load, store):
    size = from_ref.shape[0] // 4
    rows = [pl.ds(i * size, size) for i in range(4)]
    loads = [pltpu.make_async_copy(from_ref.at[at, :], room.at[at, :], load.at[i]) for i, at in enumerate(rows)]
    stores = [pltpu.make_async_copy(room.at[at, :], to_ref.at[at, :], store.at[i]) for i, at in enumerate(rows)]
    for copy in loads:
        copy.start()
    for copy, then in zip(loads, stores):
        copy.wait()
        then.start()
    for copy in stores:
        copy.wait()


def solution(mesh):
    n = mesh.shape["tp"]

    def step(x, gain, wq, wk, wv, wo):
        mine, depth = x.shape
        width = wq.shape[1]
        heads, tiles, rows = width // HEAD, depth // TILE, mine * n
        anywhere = pl.BlockSpec(memory_space=pl.ANY)
        dma = pltpu.SemaphoreType.DMA
        y = pl.pallas_call(
            functools.partial(kernel, n),
            out_shape=jax.ShapeDtypeStruct((mine, depth), bf16),
            in_specs=[anywhere, pl.BlockSpec(memory_space=pltpu.VMEM)] + [anywhere] * 5,
            out_specs=anywhere,
            scratch_shapes=[
                pltpu.VMEM((mine, depth), bf16),
                pltpu.VMEM((rows, 2 * HEAD), f32),
                pltpu.VMEM((tiles, rows, TILE), bf16),
                pltpu.VMEM((SLOTS * TILE, 3 * width), bf16),
                pltpu.VMEM((512, 3 * width), f32),
                pltpu.VMEM((3 * heads, rows, HEAD), bf16),
                pltpu.VMEM((256, width), bf16),
                pltpu.VMEM((16, HEAD), f32),
                pltpu.VMEM((heads, HEAD + 8, 128), f32),
                dma((2,)), dma((SLOTS, 3)), dma((6,)), dma((tiles,)),
                dma((tiles,)), dma((tiles,)), dma((3, tiles)), dma((3, tiles)), dma((3, tiles)), dma((3, tiles)),
                dma((4, tiles)), dma((4, tiles)), dma((3, tiles)), dma((3, tiles)),
                pltpu.SemaphoreType.REGULAR((5,)),
            ],
            compiler_params=pltpu.CompilerParams(collective_id=0, has_side_effects=True, vmem_limit_bytes=VMEM),
        )(x, gain, jnp.asarray(rotation(rows)), wq, wk, wv, wo)
        return pl.pallas_call(
            handed_on,
            out_shape=jax.ShapeDtypeStruct((mine, depth), bf16),
            in_specs=[anywhere],
            out_specs=anywhere,
            scratch_shapes=[pltpu.VMEM((mine, depth), bf16), dma((4,)), dma((4,))],
        )(y)

    tokens, columns = P(("dp", "tp"), None), P(None, "tp")
    return jax.shard_map(
        step,
        mesh=mesh,
        in_specs=(tokens, P(None), columns, columns, columns, P("tp", None)),
        out_specs=tokens,
        check_vma=False,
    )
```

```python
import functools

import jax
import jax.numpy as jnp
import numpy as np
from jax import lax
from jax.experimental import pallas as pl
from jax.experimental.pallas import tpu as pltpu
from jax.sharding import PartitionSpec as P

HEAD = 128
THETA = 10000
LOG2E = 1.4426950408889634
HIDDEN = -2e30
VMEM = 63 * 2**20
CORES = 2
TILE = 1024
SLOTS = 3
LAG = 3
MESH = pl.DeviceIdType.MESH
f32, bf16 = jnp.float32, jnp.bfloat16

INTO = (640, 256, 384)
EXCHANGED = (512, 768, 896, None)


def rotation(rows):
    half = HEAD // 2
    angle = np.arange(rows, dtype=np.float64)[:, None] * float(THETA) ** (-np.arange(half, dtype=np.float64) / half)
    cos, sin = np.cos(angle), np.sin(angle)
    return np.concatenate([cos, cos, -sin, sin], 1).astype(np.float32)


def pick(i, values):
    got = values[-1]
    for m in range(len(values) - 2, -1, -1):
        got = jnp.where(i == m, values[m], got)
    return got


def kernel(n, x_ref, gain_ref, turn_ref, wq_ref, wk_ref, wv_ref, wo_ref, y_ref,
           x_s, turn_s, held, ring, acc, qkv, seen, top_s, mix_s,
           in_sem, w_sem, wo_sem, y_sem, own_send, own_recv, to_send, to_recv, pass_send, pass_recv, ex_send, ex_recv, rs_send, rs_recv, free):
    me = lax.axis_index("tp")
    chips = n // CORES
    chip, core = me // CORES, me % CORES
    chip_at = lambda ahead: lax.rem(chip + ahead, chips)
    partner = chip * CORES + 1 - core
    forth, back = jnp.where(core == 0, 1, chips - 1), jnp.where(core == 0, chips - 1, 1)
    after, before = chip_at(forth) * CORES + core, chip_at(back) * CORES + core
    across = chip_at(forth) * CORES + 1 - core
    own = pl.multiple_of(core * 128, 128)
    other = pl.multiple_of((1 - core) * 128, 128)
    tiles = x_ref.shape[1] // TILE
    width = wq_ref.shape[1]
    heads = width // HEAD
    early = ((core == 0) & (chip != 0)) | ((core == 1) & (chip == chips - 1))

    def cols(j, size=TILE):
        return pl.ds(pl.multiple_of(j * size, 128), size)

    def some(r, size=128):
        return pl.ds(pl.multiple_of(r, 128), size)

    def weights(j):
        slot = lax.rem(j, SLOTS)
        return [pltpu.make_async_copy(w.at[cols(j), :], ring.at[some(slot * TILE, TILE), pl.ds(m * width, width)], w_sem.at[slot, m])
                for m, w in enumerate((wq_ref, wk_ref, wv_ref))]

    def wo_slot(i, depth):
        slot = lax.rem(i, depth)
        return some(slot // 3 * width, width), cols(lax.rem(slot, 3))

    def wo_tile(i, depth):
        rows, columns = wo_slot(i, depth)
        return pltpu.make_async_copy(wo_ref.at[:, cols(lax.rem(i, tiles))], ring.at[rows, columns], wo_sem.at[lax.rem(i, depth)])

    def remote(j, at, to, send, recv, device):
        return pltpu.make_async_remote_copy(src_ref=held.at[j, some(at), :], dst_ref=held.at[j, some(to), :], send_sem=send, recv_sem=recv,
                                            device_id={"tp": device}, device_id_type=MESH)

    def own_to_partner(j):
        return remote(j, own, own, own_send.at[j], own_recv.at[j], partner)

    def message(s, j):
        first = 256 + own
        at = (own, jnp.where(early, first, other), jnp.where(early, other, first))[s]
        return remote(j, at, 256 + s * 256 + own, to_send.at[s, j], to_recv.at[s, j], after)

    def passed(s, j, core_at=own):
        return remote(j, 256 + s * 256 + core_at, 256 + s * 256 + core_at, pass_send.at[s, j], pass_recv.at[s, j], partner)

    def exchange(b, j):
        return remote(j, own, pick(b, [own if r is None else r for r in EXCHANGED]), ex_send.at[b, j], ex_recv.at[b, j], partner)

    def exchanged(b):
        return some(pick(b, [other if r is None else r for r in EXCHANGED]))

    def onwards(kind, j):
        at = EXCHANGED[kind]
        return remote(j, at, INTO[kind], rs_send.at[kind, j], rs_recv.at[kind, j], after if kind < 2 else across)

    def arrival(kind, j):
        return remote(j, EXCHANGED[0], pick(kind, INTO), rs_send.at[kind, j], rs_recv.at[kind, j], after)

    def out(j):
        return pltpu.make_async_copy(held.at[j, some(own), :], y_ref.at[:, cols(j)], y_sem.at[j])

    fetch = pltpu.make_async_copy(x_ref, x_s, in_sem.at[0])
    fetch.start()
    for j in range(SLOTS):
        for copy in weights(j):
            copy.start(priority=1)
    fetch_turn = pltpu.make_async_copy(turn_ref, turn_s, in_sem.at[1])
    fetch_turn.start()
    barrier = pltpu.get_barrier_semaphore()
    for device in (partner, after, before, across):
        pl.semaphore_signal(barrier, inc=1, device_id={"tp": device}, device_id_type=MESH)
    fetch.wait()
    total = jnp.zeros((128, 128), f32)
    for j in range(tiles):
        wide = x_s[:, j * TILE : (j + 1) * TILE].astype(f32)
        square = wide * wide
        for m in range(0, TILE, 128):
            total = total + square[:, m : m + 128]
    scale = lax.rsqrt(jnp.sum(total, -1, keepdims=True) / x_ref.shape[1] + 1e-6)

    def norm(j, _):
        wide = x_s[:, cols(j)].astype(f32)
        held[j, some(own), :] = (wide * scale * gain_ref[cols(j)].astype(f32)).astype(bf16)
        return 0

    lax.fori_loop(0, tiles, norm, 0)
    pl.semaphore_wait(barrier, 4)

    def send(j, _):
        own_to_partner(j).start()
        message(0, j).start()
        return 0

    lax.fori_loop(0, tiles, send, 0)

    def unit(j, first, into, fresh):
        w = ring[some(lax.rem(j, SLOTS) * TILE, TILE), :]
        term = jnp.dot(held[j, first : first + 256, :], w, preferred_element_type=f32)
        acc[into : into + 256, :] = jnp.where(fresh, 0.0, acc[into : into + 256, :]) + term

    def turned_head(h, into, blocks):
        for half, t_at in enumerate(blocks):
            rows = some(t_at * 128)
            cos, sin = turn_s[rows, :HEAD], turn_s[rows, HEAD:]
            for m in range(3):
                t = acc[into + half * 128 : into + half * 128 + 128, cols(m * heads + h, HEAD)].astype(bf16)
                if m < 2:
                    t = t.astype(f32)
                    t = (t * cos + pltpu.roll(t, HEAD // 2, 1) * sin).astype(bf16)
                qkv[m * heads + h, rows, :] = t

    def turned_heads(into, blocks):
        lax.fori_loop(0, heads, lambda h, _: turned_head(h, into, blocks), None, unroll=heads)

    def arrivals(s):
        p, q = chip_at(chips - 1), chip_at(1)
        p_first, q_first = 2 * lax.rem(p + chips - 1, chips), 2 * lax.rem(q + 1, chips) + 1
        return [(2 * p, 2 * q + 1),
                (jnp.where(p != 0, p_first, 2 * p + 1), jnp.where(q == chips - 1, q_first, 2 * q)),
                (jnp.where(p != 0, 2 * p + 1, p_first), jnp.where(q == chips - 1, 2 * q, q_first))][s]

    def came(s, j):
        message(s, j).wait_recv()
        passed(s, j).start()

    def first_came(j):
        came(0, j)

        @pl.when(early)
        def _():
            message(1, j).start()

    def refill(j, more):
        @pl.when(more)
        def _():
            for copy in weights(lax.rem(j + SLOTS, tiles)):
                copy.start(priority=1)

    def own_chip(j, _):
        own_to_partner(j).wait_recv()

        @pl.when(jnp.logical_not(early))
        def _():
            message(1, j).start()

        @pl.when(j >= 3)
        def _():
            first_came(j - 3)

        for copy in weights(j):
            copy.wait()
        unit(j, 0, 0, j == 0)
        refill(j, True)
        return 0

    lax.fori_loop(0, tiles, own_chip, 0)
    fetch_turn.wait()

    def first_arrivals(j, _):
        @pl.when(j < 3)
        def _():
            first_came(j + tiles - 3)

        message(2, j).start()

        @pl.when(j >= 5)
        def _():
            came(1, j - 5)

        passed(0, j, other).wait_recv()
        for copy in weights(j):
            copy.wait()
        turned_head(j, 0, (2 * chip, 2 * chip + 1))
        unit(j, 256, 256, j == 0)
        refill(j, True)
        return 0

    lax.fori_loop(0, tiles, first_arrivals, 0)

    def second_arrivals(j, _):
        @pl.when((j >= 3) & (j + 1 < tiles))
        def _():
            came(1, j + 1)

        passed(1, j, other).wait_recv()
        for copy in weights(j):
            copy.wait()
        turned_head(j, 256, arrivals(0))
        unit(j, 512, 0, j == 0)
        refill(j, j + SLOTS < tiles)
        return 0

    lax.fori_loop(0, tiles, second_arrivals, 0)
    for i in range(3):
        wo_tile(i, 3).start(priority=1)
    for copy in weights(2):
        copy.start(priority=1)

    def sent_first(j, _):
        own_to_partner(j).wait_send()
        message(0, j).wait_send()
        passed(1, j).wait_send()
        return 0

    lax.fori_loop(0, tiles, sent_first, 0)
    for i, device in enumerate((partner, before)):
        pl.semaphore_signal(free.at[i], inc=1, device_id={"tp": device}, device_id_type=MESH)
    turned_heads(0, arrivals(1))

    e = HEAD**-0.5 * LOG2E

    def dot(a, b, ca, cb):
        return lax.dot_general(a, b, (((ca,), (cb,)), ((), ())), preferred_element_type=f32)

    def attention(t, into):
        queries = some(t * 128)

        def block(at, size, seen_before, diagonal):
            keys = some(at, size)
            scores = [dot(qkv[heads + h, keys, :], qkv[h, queries, :], 1, 1) for h in range(heads)]
            weights, keeps = [], []
            for h, s in enumerate(scores):
                if diagonal:
                    key = lax.broadcasted_iota(jnp.int32, (size, 128), 0)
                    s = jnp.where(lax.broadcasted_iota(jnp.int32, (size, 128), 1) + (size - 128) >= key, s, HIDDEN)
                top = s.max(axis=0, keepdims=True)
                if seen_before:
                    old = top_s[h : h + 1, :]
                    top = jnp.maximum(old, top)
                    keeps.append(jnp.exp2((old - top) * e))
                top_s[h : h + 1, :] = top
                weights.append(jnp.exp2((s - top) * e).astype(bf16))
            for h, p in enumerate(weights):
                values = jnp.concatenate([qkv[2 * heads + h, keys, :].T, jnp.ones((8, size), bf16)], axis=0)
                got = dot(values, p, 1, 0)
                mix_s[h] = mix_s[h] * keeps[h] + got if seen_before else got

        @pl.when(t % 2 == 0)
        def _():
            block(t * 128, 128, False, True)

        @pl.when(t % 2 == 1)
        def _():
            block((t - 1) * 128, 256, False, True)

        lax.fori_loop(0, t // 2, lambda j, _: block(j * 256, 256, True, False), None)
        for h in range(heads):
            got = (mix_s[h, :HEAD, :] * (1 / mix_s[h, HEAD : HEAD + 1, :])).T.astype(bf16)
            seen[some(into), h * HEAD : (h + 1) * HEAD] = got

    far, right, left = chip_at(2), chip_at(1), chip_at(chips - 1)
    got_far_first = ((core == 0) & (chip == chips - 1)) | ((core == 1) & (chip != 0))
    into_far = jnp.where(got_far_first, 0, 1)

    def blocks_of(b):
        right_far, left_far = chip == chips // 2, chip != 1
        to_right = pick(b, [jnp.where(right_far, 2 * far + 1, 2 * right), jnp.where(right_far, 2 * right, 2 * far + 1), 2 * right + 1, 2 * chip])
        to_left = pick(b, [jnp.where(left_far, 2 * far, 2 * left + 1), jnp.where(left_far, 2 * left + 1, 2 * far), 2 * left, 2 * chip + 1])
        return jnp.where(core == 0, to_right, to_left), jnp.where(core == 0, to_left, to_right)

    def place(i):
        return pl.ds(pl.multiple_of(i // 3 * 64, 64), 64), cols(lax.rem(i, 3))

    def wait_tile(b, j, i, depth):
        wo_tile(i, depth).wait()

        @pl.when(b > 0)
        def _():
            exchange(b - 1, j).wait_send()

    def tile(b, j, i, depth):
        rows, columns = wo_slot(i, depth)
        term = jnp.dot(seen[...], ring[rows, columns], preferred_element_type=f32)
        for half in range(2):
            acc[place(18 + lax.rem(j, 3) * 2 + half)] = term[half * 64 : half * 64 + 64]
        held[j, some(own), :] = term[128:].astype(bf16)

    def send_tile(b, j, i, count, depth):
        exchange(b, j).start()

        @pl.when(i + depth < count)
        def _():
            wo_tile(i + depth, depth).start(priority=1)

    def add(b, j):
        at = exchanged(b)
        got = held[j, at, :].astype(f32)
        low = acc[place(18 + lax.rem(j, 3) * 2)] + got[:64]
        high = acc[place(18 + lax.rem(j, 3) * 2 + 1)] + got[64:]
        held[j, at, :] = jnp.concatenate([low, high], 0).astype(bf16)
        if not isinstance(b, int):
            acc[place(2 * j)] = low
            acc[place(2 * j + 1)] = high

    def send_sum(b, j):
        for kind in range(2):

            @pl.when(b == kind)
            def _():
                onwards(kind, j).start()

        @pl.when(b == 2)
        def _():
            arrival(into_far, j).wait_recv()
            more = held[j, some(pick(into_far, INTO)), :].astype(f32)
            at = EXCHANGED[2]
            held[j, at : at + 64, :] = (acc[place(2 * j)] + more[:64]).astype(bf16)
            held[j, at + 64 : at + 128, :] = (acc[place(2 * j + 1)] + more[64:]).astype(bf16)
            onwards(2, j).start()

    def finish(b, j):
        exchange(b, j).wait_recv()
        add(b, j)
        send_sum(b, j)

    def tiles_of(b, first, count, depth, besides):
        def begin(j, _):
            wait_tile(b, j, first + j, depth)
            tile(b, j, first + j, depth)
            send_tile(b, j, first + j, count, depth)
            return 0

        def go_on(j, _):
            wait_tile(b, j, first + j, depth)
            exchange(b, j - LAG).wait_recv()
            add(b, j - LAG)
            tile(b, j, first + j, depth)
            send_tile(b, j, first + j, count, depth)
            send_sum(b, j - LAG)
            besides(j)
            return 0

        lax.fori_loop(0, LAG, begin, 0)
        lax.fori_loop(LAG, tiles, go_on, 0)

    def attend(b):
        mine, others = blocks_of(b)

        def one(i, _):
            attention(jnp.where(i == 0, mine, others), i * 128)
            return 0

        lax.fori_loop(0, 2, one, 0)

    attend(0)
    for i in range(2):
        pl.semaphore_wait(free.at[i], 1)

    def also_came(j):
        @pl.when(j >= 3)
        def _():
            came(2, j - 3)

    tiles_of(0, 0, tiles, 3, also_came)
    for j in (3, 4):
        for copy in weights(j):
            copy.start(priority=1)

    def last_arrivals(i, _):
        j = lax.rem(i + 2, tiles)

        @pl.when(i < 3)
        def _():
            came(2, i + tiles - 3)

        @pl.when(i < LAG)
        def _():
            finish(0, i + tiles - LAG)

        passed(2, j, other).wait_recv()
        for copy in weights(j):
            copy.wait()
        unit(j, 768, 0, i == 0)
        refill(j, i + SLOTS < tiles)
        return 0

    lax.fori_loop(0, tiles, last_arrivals, 0)
    for i in range(6):
        wo_tile(i, 6).start(priority=1)

    def sent(j, _):
        for s in (1, 2):
            message(s, j).wait_send()
        for s in (0, 2):
            passed(s, j).wait_send()
        return 0

    lax.fori_loop(0, tiles, sent, 0)
    for i, device in enumerate((partner, before, across)):
        pl.semaphore_signal(free.at[2 + i], inc=1, device_id={"tp": device}, device_id_type=MESH)
    turned_heads(0, arrivals(2))

    def later_step(b, _):
        attend(b)

        @pl.when(b == 1)
        def _():
            for i in range(3):
                pl.semaphore_wait(free.at[2 + i], 1)

        tiles_of(b, (b - 1) * tiles, 3 * tiles, 6, lambda j: None)
        lax.fori_loop(tiles - LAG, tiles, lambda j, _: finish(b, j), None)
        return 0

    lax.fori_loop(1, 4, later_step, 0)

    def last(j, _):
        exchange(3, j).wait_send()
        arrival(1 - into_far, j).wait_recv()
        arrival(2, j).wait_recv()
        near = held[j, some(pick(1 - into_far, INTO)), :].astype(f32)
        for half in range(2):
            rows = slice(half * 64, half * 64 + 64)
            total = acc[place(2 * j + half)] + near[rows] + held[j, INTO[2] + half * 64 : INTO[2] + half * 64 + 64, :].astype(f32)
            held[j, pl.ds(pl.multiple_of(own + half * 64, 64), 64), :] = (x_s[rows, cols(j)].astype(f32) + total).astype(bf16)
        out(j).start()
        return 0

    lax.fori_loop(0, tiles, last, 0)

    def done(j, _):
        for kind in range(3):
            onwards(kind, j).wait_send()
        out(j).wait()
        return 0

    lax.fori_loop(0, tiles, done, 0)


def handed_on(from_ref, to_ref, room, load, store):
    size = from_ref.shape[0] // 4
    rows = [pl.ds(i * size, size) for i in range(4)]
    loads = [pltpu.make_async_copy(from_ref.at[at, :], room.at[at, :], load.at[i]) for i, at in enumerate(rows)]
    stores = [pltpu.make_async_copy(room.at[at, :], to_ref.at[at, :], store.at[i]) for i, at in enumerate(rows)]
    for copy in loads:
        copy.start()
    for copy, then in zip(loads, stores):
        copy.wait()
        then.start()
    for copy in stores:
        copy.wait()


def solution(mesh):
    n = mesh.shape["tp"]

    def step(x, gain, wq, wk, wv, wo):
        mine, depth = x.shape
        width = wq.shape[1]
        heads, tiles, rows = width // HEAD, depth // TILE, mine * n
        anywhere = pl.BlockSpec(memory_space=pl.ANY)
        dma = pltpu.SemaphoreType.DMA
        y = pl.pallas_call(
            functools.partial(kernel, n),
            out_shape=jax.ShapeDtypeStruct((mine, depth), bf16),
            in_specs=[anywhere, pl.BlockSpec(memory_space=pltpu.VMEM)] + [anywhere] * 5,
            out_specs=anywhere,
            scratch_shapes=[
                pltpu.VMEM((mine, depth), bf16),
                pltpu.VMEM((rows, 2 * HEAD), f32),
                pltpu.VMEM((tiles, rows, TILE), bf16),
                pltpu.VMEM((SLOTS * TILE, 3 * width), bf16),
                pltpu.VMEM((512, 3 * width), f32),
                pltpu.VMEM((3 * heads, rows, HEAD), bf16),
                pltpu.VMEM((256, width), bf16),
                pltpu.VMEM((16, HEAD), f32),
                pltpu.VMEM((heads, HEAD + 8, 128), f32),
                dma((2,)), dma((SLOTS, 3)), dma((6,)), dma((tiles,)),
                dma((tiles,)), dma((tiles,)), dma((3, tiles)), dma((3, tiles)), dma((3, tiles)), dma((3, tiles)),
                dma((4, tiles)), dma((4, tiles)), dma((3, tiles)), dma((3, tiles)),
                pltpu.SemaphoreType.REGULAR((5,)),
            ],
            compiler_params=pltpu.CompilerParams(collective_id=0, has_side_effects=True, vmem_limit_bytes=VMEM),
        )(x, gain, jnp.asarray(rotation(rows)), wq, wk, wv, wo)
        return pl.pallas_call(
            handed_on,
            out_shape=jax.ShapeDtypeStruct((mine, depth), bf16),
            in_specs=[anywhere],
            out_specs=anywhere,
            scratch_shapes=[pltpu.VMEM((mine, depth), bf16), dma((4,)), dma((4,))],
        )(y)

    tokens, columns = P(("dp", "tp"), None), P(None, "tp")
    return jax.shard_map(
        step,
        mesh=mesh,
        in_specs=(tokens, P(None), columns, columns, columns, P("tp", None)),
        out_specs=tokens,
        check_vma=False,
    )
```
